32 devices in a mesh: grp: 2 (over x), sec: 16 (over z, y, core).
Axes of the slice: x: 2, y: 2, z: 4, core: 2. Of those that a mesh axis runs over, the one named last changes fastest.
Arguments:
- section_tile: bfloat16 [32, 512, 512], P(('grp', 'sec')), parts along dimension 0, may hold values from -8 to 8
- placement: int32 [64, 2], P('grp'), parts along dimension 0, may hold values from 0 to 384
- tissue_mask: int32 [32, 32], P(('grp', 'sec')), parts along dimension 0, may hold values 0 or 1
- level_use: int32 [3, 64], P(None, 'grp'), parts along dimension 1, may hold values 0 or 1
Outputs:
- flow_next: float32 [32, 2, 32], P(('grp', 'sec')), parts along dimension 0
- flow_skip: float32 [32, 2, 32], P(('grp', 'sec')), parts along dimension 0
- position: float32 [32, 2, 32], P(('grp', 'sec')), parts along dimension 0
The draws below stay inside these ranges and needn't reach their ends.
There are 2 independent parts, one for each index of `grp`. The reference program is written for one: setup_inputs(seed, part) draws one part's arguments, and reference() takes and returns one part's arrays. A program takes and returns all parts, laid end to end along the dimension named above; each array names one. Nothing has to cross between parts.
All inputs are finite; a program needn't handle non-finite values. No bound on the sum of `tissue_mask` on one device may be relied on, other than what follows from the above.
Results may differ from the reference program's by a relative error of at most 0.0044.
Values may be sent and summed in bfloat16 or wider, within the bound.
No kernel may reach another device: no remote copies, remote signals or barrier semaphores. Data moves between devices by JAX's collectives and lax.ppermute only.
A program may use at most 128 MiB of HBM per device.

```python
import jax
import jax.numpy as jnp
from jax import lax

PATCH = 128
LEVELS = 3
P_SIZE = 32
TILE = 512
SEC = 16


def draw_section_tile(key, part):
    base_key = jax.random.fold_in(key, 11)
    shift_key = jax.random.fold_in(key, 12)
    noise_key = jax.random.fold_in(key, 13)
    offsets = jax.random.randint(shift_key, (SEC, 2), -4, 5)
    base = jax.random.normal(base_key, (TILE, TILE), jnp.float32)
    noise = 0.3 * jax.random.normal(noise_key, (SEC, TILE, TILE), jnp.float32)

    def one_section(offset, fresh):
        moved = jnp.roll(base, offset[0], axis=0)
        moved = jnp.roll(moved, offset[1], axis=1)
        return moved + fresh
    tiles = jax.vmap(one_section)(offsets, noise)
    return jnp.clip(tiles, -8.0, 8.0).astype(jnp.bfloat16)


def set_ends(values, key, least, top_value):
    place = [jax.random.randint(jax.random.fold_in(key, axis), (), 0, length) for axis, length in enumerate(values.shape)]
    widest = values.shape.index(max(values.shape))
    beside = place[:widest] + [(place[widest] + 1) % values.shape[widest]] + place[widest + 1:]
    return values.at[tuple(place)].set(least).at[tuple(beside)].set(top_value)


def setup_inputs(seed: int = 0, part: int = 0) -> dict:
    key_list = jax.random.split(jax.random.key(seed), 5)
    part_splits = jax.random.split(jax.random.fold_in(key_list[4], part), 5)
    section_tile = draw_section_tile(jax.random.fold_in(jax.random.fold_in(key_list[4], part), 71), part)
    placement = set_ends(jax.random.randint(part_splits[1], (P_SIZE, 2), 0, TILE - PATCH + 1), jax.random.fold_in(part_splits[1], 1), 0, TILE - PATCH).astype(jnp.int32)
    tissue_mask = set_ends((jax.random.randint(part_splits[2], (SEC, P_SIZE), 0, 4) < 3).astype(jnp.int32), jax.random.fold_in(part_splits[2], 1), 0, 1)
    level_use = set_ends((jax.random.randint(part_splits[3], (LEVELS, P_SIZE), 0, 3) < 2).astype(jnp.int32), jax.random.fold_in(part_splits[3], 1), 0, 1)
    return {"section_tile": section_tile, "placement": placement, "tissue_mask": tissue_mask, "level_use": level_use}


def dft_tables():
    index = jnp.arange(PATCH, dtype=jnp.int32)
    product = (index[:, None] * index[None, :]) % PATCH
    angles = product.astype(jnp.float32) * (2.0 * jnp.pi / PATCH)
    return jnp.cos(angles).astype(jnp.bfloat16), (-jnp.sin(angles)).astype(jnp.bfloat16)


def band_vector(level_number):
    index = jnp.arange(PATCH, dtype=jnp.int32)
    signed_freq = jnp.minimum(index, PATCH - index)
    return (signed_freq < PATCH // 2 ** (level_number + 1)).astype(jnp.float32)


def offset_vector():
    index = jnp.arange(PATCH, dtype=jnp.int32)
    return jnp.where(index < PATCH // 2, index, index - PATCH).astype(jnp.float32)


def extract(plane, placement):
    def one_patch(corner):
        return lax.dynamic_slice(plane, (corner[0], corner[1]), (PATCH, PATCH))
    return jax.vmap(one_patch)(placement.astype(jnp.int32))


def blend_terms(form, left, right):
    return jnp.einsum(form, left.astype(jnp.float32), right.astype(jnp.float32))


def spectrum(patches, cosine_lookup, sine_lookup):
    real_rows = blend_terms("kn,pnm->pkm", cosine_lookup, patches).astype(jnp.bfloat16)
    imag_rows = blend_terms("kn,pnm->pkm", sine_lookup, patches).astype(jnp.bfloat16)
    spec_real = (blend_terms("pkm,ml->pkl", real_rows, cosine_lookup) - blend_terms("pkm,ml->pkl", imag_rows, sine_lookup)) / PATCH
    spec_imag = (blend_terms("pkm,ml->pkl", real_rows, sine_lookup) + blend_terms("pkm,ml->pkl", imag_rows, cosine_lookup)) / PATCH
    return spec_real.astype(jnp.bfloat16), spec_imag.astype(jnp.bfloat16)


def centroid(correl, offsets):
    weights = correl * correl
    total = jnp.sum(weights, axis=(1, 2)) + 1e-6
    along_rows = jnp.sum(weights * offsets[None, :, None], axis=(1, 2)) / total
    along_cols = jnp.sum(weights * offsets[None, None, :], axis=(1, 2)) / total
    return jnp.stack([along_rows, along_cols])


def pair_flow(own_real, own_imag, other_real, other_imag, cosine_lookup, sine_lookup, usage, valid):
    first_real = own_real.astype(jnp.float32)
    first_imag = own_imag.astype(jnp.float32)
    second_real = other_real.astype(jnp.float32)
    second_imag = other_imag.astype(jnp.float32)
    cross_power_real = (first_real * second_real + first_imag * second_imag).astype(jnp.bfloat16)
    cross_power_imaginary = (first_imag * second_real - first_real * second_imag).astype(jnp.bfloat16)
    offsets = offset_vector()
    estimate = jnp.zeros((2, usage.shape[1]), jnp.float32)
    for level_number in range(LEVELS):
        band_row = band_vector(level_number)
        window = band_row[:, None] * band_row[None, :]
        tissue_real = cross_power_real.astype(jnp.float32) * window
        tissue_imaginary = cross_power_imaginary.astype(jnp.float32) * window
        partial_real = (blend_terms("dt,hts->hds", cosine_lookup, tissue_real) + blend_terms("dt,hts->hds", sine_lookup, tissue_imaginary)).astype(jnp.bfloat16)
        partial_imaginary = (blend_terms("dt,hts->hds", cosine_lookup, tissue_imaginary) - blend_terms("dt,hts->hds", sine_lookup, tissue_real)).astype(jnp.bfloat16)
        correl = (blend_terms("pkq,ql->pkl", partial_real, cosine_lookup) + blend_terms("pkq,ql->pkl", partial_imaginary, sine_lookup)) / PATCH
        estimate = estimate + usage[level_number][None, :] * centroid(correl, offsets)
    count = jnp.maximum(jnp.sum(usage, axis=0), 1.0)
    return valid[None, :] * estimate / count[None, :]


def shifted(values, step):
    padding = jnp.zeros_like(values[:step])
    return jnp.concatenate([values[step:], padding], axis=0)


def reference(section_tile, placement, tissue_mask, level_use):
    cosine_lookup, sine_lookup = dft_tables()

    def section_spectra(plane):
        return spectrum(extract(plane, placement), cosine_lookup, sine_lookup)

    spec_real, spec_imag = lax.map(section_spectra, section_tile)
    flags = tissue_mask.astype(jnp.float32)
    usage = level_use.astype(jnp.float32)

    def flows_at(step):
        def one_section(items):
            own_real, own_imag, other_real, other_imag, own_flag, other_flag = items
            return pair_flow(own_real, own_imag, other_real, other_imag, cosine_lookup, sine_lookup, usage, own_flag * other_flag)
        return lax.map(one_section, (spec_real, spec_imag, shifted(spec_real, step), shifted(spec_imag, step), flags, shifted(flags, step)))

    flow_next = flows_at(1)
    flow_skip = flows_at(2)
    position = jnp.cumsum(flow_next, axis=0)
    return flow_next, flow_skip, position
```

```python
import functools

import jax
import jax.numpy as jnp
import numpy as np
from jax import lax
from jax.experimental import pallas as pl
from jax.experimental.pallas import tpu as pltpu
from jax.sharding import PartitionSpec as P

PATCH = 128
LEVELS = 3
HALF = PATCH // 2
QUAD = 4


def tables():
    index = np.arange(PATCH)
    angles = ((index[:, None] * index[None, :]) % PATCH).astype(np.float32) * np.float32(2.0 * np.pi / PATCH)
    cosine = np.cos(angles).astype(jnp.bfloat16).astype(np.float32)
    sine = (-np.sin(angles)).astype(jnp.bfloat16).astype(np.float32)
    zero = np.zeros((PATCH, HALF), np.float32)
    window = np.zeros((4, 3 * PATCH, PATCH), np.float32)
    cos_half, sin_half = cosine[:, :HALF], sine[:, :HALF]
    for place, part in enumerate(
        ([cos_half, zero], [sin_half, zero], [zero, cos_half], [zero, sin_half])
    ):
        window[place, PATCH : 2 * PATCH] = np.concatenate(part, axis=1)
    forward = np.concatenate([cosine, sine], axis=1) / PATCH
    inverse_rows = np.zeros((LEVELS * 2 * PATCH, 2 * PATCH), np.float32)
    inverse_cols = np.zeros((LEVELS, 2 * PATCH, 2 * PATCH), np.float32)
    signed = np.minimum(index, PATCH - index)
    twice = np.where(np.arange(HALF) == 0, 1.0, 2.0)[:, None]
    for level in range(LEVELS):
        band = (signed < PATCH // 2 ** (level + 1)).astype(np.float32)
        cos_left, sin_left = cosine * band[None, :], sine * band[None, :]
        top = 2 * PATCH * level
        inverse_rows[top : top + PATCH] = np.concatenate([cos_left, sin_left], axis=1)
        inverse_rows[top + PATCH : top + 2 * PATCH] = np.concatenate([-sin_left, cos_left], axis=1)
        weight = twice * band[:HALF, None] / PATCH
        cos_right, sin_right = cosine[:HALF] * weight, sine[:HALF] * weight
        for member in range(2):
            cols = slice(member * PATCH, (member + 1) * PATCH)
            inverse_cols[level, member * HALF : (member + 1) * HALF, cols] = cos_right
            inverse_cols[level, PATCH + member * HALF : PATCH + (member + 1) * HALF, cols] = sin_right
    offset = np.where(index < HALF, index, index - PATCH).astype(np.float32)
    moments = np.zeros((8, PATCH), np.float32)
    moments[0] = 1.0
    moments[1] = offset
    offset_rows = np.broadcast_to(offset[:, None], (PATCH, PATCH)).copy()
    return (
        jnp.asarray(window),
        jnp.asarray(forward, jnp.bfloat16),
        jnp.asarray(inverse_rows, jnp.bfloat16),
        jnp.asarray(inverse_cols, jnp.bfloat16),
        jnp.asarray(moments),
        jnp.asarray(offset_rows),
    )


def product(left, right):
    return jnp.dot(left, right, preferred_element_type=jnp.float32)


def fill_panels(tile_ref, panels):
    for panel in range(panels.shape[0]):
        panels[panel] = tile_ref[:, panel * PATCH : (panel + 1) * PATCH].astype(jnp.float32)


def pair_spectrum(pair, place_ref, panels, window_ref, forward):
    last = panels.shape[0] - 2
    total = None
    for member in range(2):
        row = place_ref[2 * pair + member, 0]
        col = place_ref[2 * pair + member, 1]
        panel = jnp.minimum(col // PATCH, last)
        shift = col - panel * PATCH
        patch = jnp.concatenate(
            [panels[panel, pl.ds(row, PATCH), :], panels[panel + 1, pl.ds(row, PATCH), :]], axis=1
        ).astype(jnp.bfloat16)
        table = jnp.concatenate(
            [
                window_ref[2 * member, pl.ds(PATCH - shift, 2 * PATCH), :],
                window_ref[2 * member + 1, pl.ds(PATCH - shift, 2 * PATCH), :],
            ],
            axis=1,
        ).astype(jnp.bfloat16)
        term = product(patch, table)
        total = term if total is None else total + term
    cols = total.astype(jnp.bfloat16)
    turned = jnp.concatenate([-cols[:, PATCH:], cols[:, :PATCH]], axis=1)
    return product(forward, jnp.concatenate([cols, turned], axis=0)).astype(jnp.bfloat16)


def spectrum_kernel(place_ref, tile_ref, window_ref, forward_ref, spec_ref, panels):
    fill_panels(tile_ref, panels)
    forward = forward_ref[...]

    def step(pair, carry):
        spec_ref[pair] = pair_spectrum(pair, place_ref, panels, window_ref, forward)
        return carry

    lax.fori_loop(0, spec_ref.shape[0], step, 0)


def estimate(
    place_ref, tile_ref, spec_ref, usage_ref, window_ref, forward_ref, rows_ref, cols_ref, moments_ref,
    offset_ref, panels, col_sums, row_sums,
):
    fill_panels(tile_ref, panels)

    def step(quad, carry):
        forward = forward_ref[...]
        real, imag = [], []
        for pair in range(QUAD // 2):
            other = pair_spectrum(quad * (QUAD // 2) + pair, place_ref, panels, window_ref, forward)
            own = spec_ref[quad * (QUAD // 2) + pair].astype(jnp.float32)
            other = other.astype(jnp.float32)
            own_real, own_imag = own[:, :PATCH], own[:, PATCH:]
            other_real, other_imag = other[:, :PATCH], other[:, PATCH:]
            real.append((own_real * other_real + own_imag * other_imag).astype(jnp.bfloat16))
            imag.append((own_imag * other_real - own_real * other_imag).astype(jnp.bfloat16))
        cross = jnp.concatenate([jnp.concatenate(real, axis=1), jnp.concatenate(imag, axis=1)], axis=0)
        offsets = offset_ref[...]
        offsets = jnp.concatenate([offsets, offsets], axis=1)
        for level in range(LEVELS):
            top = 2 * PATCH * level
            half = product(rows_ref[top : top + 2 * PATCH], cross).astype(jnp.bfloat16)
            for pair in range(QUAD // 2):
                lanes = slice(pair * PATCH, (pair + 1) * PATCH)
                line = jnp.concatenate([half[:PATCH, lanes], half[PATCH:, lanes]], axis=1)
                correl = product(line, cols_ref[level])
                weight = correl * correl
                by_col = jnp.sum(weight, axis=0, keepdims=True)
                by_row = jnp.sum(weight * offsets, axis=0, keepdims=True)
                for member in range(2):
                    place = quad * QUAD + 2 * pair + member
                    part = slice(member * PATCH, (member + 1) * PATCH)
                    col_sums[level, pl.ds(place, 1), :] = by_col[:, part]
                    row_sums[level, pl.ds(place, 1), :] = by_row[:, part]
        return carry

    lax.fori_loop(0, place_ref.shape[0] // QUAD, step, 0)
    usage = usage_ref[...].astype(jnp.float32)
    moments = moments_ref[...]
    across = (((1,), (1,)), ((), ()))
    along_rows, along_cols = 0.0, 0.0
    for level in range(LEVELS):
        col_part = lax.dot_general(
            moments, col_sums[level], across, precision=lax.Precision.HIGHEST,
            preferred_element_type=jnp.float32,
        )
        row_part = lax.dot_general(
            moments, row_sums[level], across, precision=lax.Precision.HIGHEST,
            preferred_element_type=jnp.float32,
        )
        scale = usage[level : level + 1] / (col_part[0:1] + 1e-6)
        along_rows = along_rows + row_part[0:1] * scale
        along_cols = along_cols + col_part[1:2] * scale
    count = jnp.maximum(jnp.sum(usage, axis=0, keepdims=True), 1.0)
    return jnp.concatenate([along_rows, along_cols], axis=0) / count


def next_kernel(*refs):
    ins, out_ref, scratch = refs[:10], refs[10], refs[11:]
    out_ref[...] = estimate(*ins, *scratch)


def skip_kernel(turn_ref, *refs):
    ins, shared_ref, outs, scratch = refs[:10], refs[10], refs[11:14], refs[14:]
    skip = estimate(*ins, *scratch)
    me = turn_ref[0]
    sections = shared_ref.shape[0]

    def mask_of(section):
        held = shared_ref[jnp.minimum(section, sections - 1), 2:3, :]
        return jnp.where(section < sections, held, jnp.zeros_like(held))

    def flow_of(section):
        return shared_ref[section, 0:2, :] * (mask_of(section) * mask_of(section + 1))

    flow_next = flow_of(me)
    outs[0][0] = flow_next
    outs[1][0] = skip * (mask_of(me) * mask_of(me + 2))
    outs[2][0] = lax.fori_loop(
        0, me, lambda section, held: held + flow_of(section), jnp.zeros_like(flow_next)
    ) + flow_next


def passed_along(block, axis, distance):
    devices = range(lax.axis_size(axis))
    route = [(i - distance, i) for i in devices if i - distance in devices]
    return lax.ppermute(block, axis, route)


def on_device(section_tile, placement, tissue_mask, level_use):
    window, forward, inverse_rows, inverse_cols, moments, offset_rows = tables()
    patches = placement.shape[0]
    side = section_tile.shape[1]
    tile = section_tile[0]
    sections = lax.axis_size("sec")
    vmem = pl.BlockSpec(memory_space=pltpu.VMEM)
    smem = pl.BlockSpec(memory_space=pltpu.SMEM)
    panels = pltpu.VMEM((side // PATCH, side, PATCH), jnp.float32)
    sums = pltpu.VMEM((LEVELS, patches, PATCH), jnp.float32)
    params = pltpu.CompilerParams(vmem_limit_bytes=24 * 2**20)

    next_tile = passed_along(tile, "sec", -1)
    own_spec = pl.pallas_call(
        spectrum_kernel,
        out_shape=jax.ShapeDtypeStruct((patches // 2, PATCH, 2 * PATCH), jnp.bfloat16),
        in_specs=[smem, vmem, vmem, vmem],
        out_specs=vmem,
        scratch_shapes=[panels],
        compiler_params=params,
        cost_estimate=pl.CostEstimate(flops=4 * 10**9, bytes_accessed=3 * 2**20, transcendentals=0),
        name="own_spectrum",
    )(placement, tile, window, forward)
    skip_tile = passed_along(next_tile, "sec", -1)

    kernel_cost = pl.CostEstimate(flops=8 * 10**9, bytes_accessed=4 * 2**20, transcendentals=0)
    shared_ins = (level_use, window, forward, inverse_rows, inverse_cols, moments, offset_rows)
    specs = [smem] + [vmem] * 9
    flow = pl.pallas_call(
        next_kernel,
        out_shape=jax.ShapeDtypeStruct((2, patches), jnp.float32),
        in_specs=specs,
        out_specs=vmem,
        scratch_shapes=[panels, sums, sums],
        compiler_params=params,
        cost_estimate=kernel_cost,
        name="flow_next",
    )(placement, next_tile, own_spec, *shared_ins)
    message = jnp.concatenate([flow, tissue_mask.astype(jnp.float32)], axis=0)
    shared = lax.all_to_all(jnp.broadcast_to(message, (sections,) + message.shape), "sec", 0, 0)
    turn = jnp.reshape(lax.axis_index("sec"), (1,)).astype(jnp.int32)
    out = jax.ShapeDtypeStruct((1, 2, patches), jnp.float32)
    return pl.pallas_call(
        skip_kernel,
        out_shape=(out, out, out),
        in_specs=[smem] + specs + [vmem],
        out_specs=(vmem, vmem, vmem),
        scratch_shapes=[panels, sums, sums],
        compiler_params=params,
        cost_estimate=kernel_cost,
        name="flow_skip",
    )(turn, placement, skip_tile, own_spec, *shared_ins, shared)


def solution(mesh):
    in_specs = (
        P(("grp", "sec"), None, None),
        P("grp", None),
        P(("grp", "sec"), None),
        P(None, "grp"),
    )
    out_specs = (
        P(("grp", "sec"), None, None),
        P(("grp", "sec"), None, None),
        P(("grp", "sec"), None, None),
    )
    return jax.shard_map(
        on_device, mesh=mesh, in_specs=in_specs, out_specs=out_specs, check_vma=False
    )
```

```python
import functools

import jax
import jax.numpy as jnp
import numpy as np
from jax import lax
from jax.experimental import pallas as pl
from jax.experimental.pallas import tpu as pltpu
from jax.sharding import PartitionSpec as P

PATCH = 128
LEVELS = 3
HALF = PATCH // 2
QUAD = 4


def tables():
    index = np.arange(PATCH)
    angles = ((index[:, None] * index[None, :]) % PATCH).astype(np.float32) * np.float32(2.0 * np.pi / PATCH)
    cosine = np.cos(angles).astype(jnp.bfloat16).astype(np.float32)
    sine = (-np.sin(angles)).astype(jnp.bfloat16).astype(np.float32)
    zero = np.zeros((PATCH, HALF), np.float32)
    window = np.zeros((4, 3 * PATCH, PATCH), np.float32)
    cos_half, sin_half = cosine[:, :HALF], sine[:, :HALF]
    for place, part in enumerate(
        ([cos_half, zero], [sin_half, zero], [zero, cos_half], [zero, sin_half])
    ):
        window[place, PATCH : 2 * PATCH] = np.concatenate(part, axis=1)
    forward = np.concatenate([cosine, sine], axis=1) / PATCH
    inverse_rows = np.zeros((LEVELS * 2 * PATCH, 2 * PATCH), np.float32)
    inverse_cols = np.zeros((LEVELS, 2 * PATCH, 2 * PATCH), np.float32)
    signed = np.minimum(index, PATCH - index)
    twice = np.where(np.arange(HALF) == 0, 1.0, 2.0)[:, None]
    for level in range(LEVELS):
        band = (signed < PATCH // 2 ** (level + 1)).astype(np.float32)
        cos_left, sin_left = cosine * band[None, :], sine * band[None, :]
        top = 2 * PATCH * level
        inverse_rows[top : top + PATCH] = np.concatenate([cos_left, sin_left], axis=1)
        inverse_rows[top + PATCH : top + 2 * PATCH] = np.concatenate([-sin_left, cos_left], axis=1)
        weight = twice * band[:HALF, None] / PATCH
        cos_right, sin_right = cosine[:HALF] * weight, sine[:HALF] * weight
        for member in range(2):
            cols = slice(member * PATCH, (member + 1) * PATCH)
            inverse_cols[level, member * HALF : (member + 1) * HALF, cols] = cos_right
            inverse_cols[level, PATCH + member * HALF : PATCH + (member + 1) * HALF, cols] = sin_right
    offset = np.where(index < HALF, index, index - PATCH).astype(np.float32)
    moments = np.zeros((8, PATCH), np.float32)
    moments[0] = 1.0
    moments[1] = offset
    return (
        jnp.asarray(window),
        jnp.asarray(forward, jnp.bfloat16),
        jnp.asarray(inverse_rows, jnp.bfloat16),
        jnp.asarray(inverse_cols, jnp.bfloat16),
        jnp.asarray(moments),
    )


def product(left, right):
    return jnp.dot(left, right, preferred_element_type=jnp.float32)


def fill_panels(tile_ref, panels):
    for panel in range(panels.shape[0]):
        panels[panel] = tile_ref[:, panel * PATCH : (panel + 1) * PATCH].astype(jnp.float32)


def pair_spectrum(pair, place_ref, panels, window_ref, forward):
    last = panels.shape[0] - 2
    total = None
    for member in range(2):
        row = place_ref[2 * pair + member, 0]
        col = place_ref[2 * pair + member, 1]
        panel = jnp.minimum(col // PATCH, last)
        shift = col - panel * PATCH
        patch = jnp.concatenate(
            [panels[panel, pl.ds(row, PATCH), :], panels[panel + 1, pl.ds(row, PATCH), :]], axis=1
        ).astype(jnp.bfloat16)
        table = jnp.concatenate(
            [
                window_ref[2 * member, pl.ds(PATCH - shift, 2 * PATCH), :],
                window_ref[2 * member + 1, pl.ds(PATCH - shift, 2 * PATCH), :],
            ],
            axis=1,
        ).astype(jnp.bfloat16)
        term = product(patch, table)
        total = term if total is None else total + term
    cols = total.astype(jnp.bfloat16)
    turned = jnp.concatenate([-cols[:, PATCH:], cols[:, :PATCH]], axis=1)
    return product(forward, jnp.concatenate([cols, turned], axis=0)).astype(jnp.bfloat16)


def spectrum_kernel(place_ref, tile_ref, window_ref, forward_ref, spec_ref, panels):
    fill_panels(tile_ref, panels)
    forward = forward_ref[...]

    def step(pair, carry):
        spec_ref[pair] = pair_spectrum(pair, place_ref, panels, window_ref, forward)
        return carry

    lax.fori_loop(0, spec_ref.shape[0], step, 0)


def estimate(
    place_ref, tile_ref, spec_ref, usage_ref, window_ref, forward_ref, rows_ref, cols_ref, moments_ref,
    panels, cross_ref, half_ref, plain, nested,
):
    fill_panels(tile_ref, panels)
    quads = place_ref.shape[0] // QUAD

    def cross_stage(quad, slot):
        forward = forward_ref[...]
        for pair in range(QUAD // 2):
            place = quad * (QUAD // 2) + pair
            other = pair_spectrum(place, place_ref, panels, window_ref, forward).astype(jnp.float32)
            own = spec_ref[place].astype(jnp.float32)
            own_real, own_imag = own[:, :PATCH], own[:, PATCH:]
            other_real, other_imag = other[:, :PATCH], other[:, PATCH:]
            lanes = slice(pair * PATCH, (pair + 1) * PATCH)
            cross_ref[slot, :PATCH, lanes] = (own_real * other_real + own_imag * other_imag).astype(jnp.bfloat16)
            cross_ref[slot, PATCH:, lanes] = (own_imag * other_real - own_real * other_imag).astype(jnp.bfloat16)

    def half_stage(slot):
        half_ref[slot] = product(rows_ref[...], cross_ref[slot]).astype(jnp.bfloat16)

    def sums_stage(quad, slot):
        for level in range(LEVELS):
            top = 2 * PATCH * level
            lines = [
                jnp.concatenate(
                    [
                        half_ref[slot, top : top + PATCH, pair * PATCH : (pair + 1) * PATCH],
                        half_ref[slot, top + PATCH : top + 2 * PATCH, pair * PATCH : (pair + 1) * PATCH],
                    ],
                    axis=1,
                )
                for pair in range(QUAD // 2)
            ]
            correl = product(jnp.concatenate(lines, axis=0), cols_ref[level])
            for pair in range(QUAD // 2):
                running, ladder = None, None
                for turn in range(PATCH // 8):
                    row = pair * PATCH + (turn * 8 + HALF) % PATCH
                    block = correl[row : row + 8]
                    weight = block * block
                    running = weight if running is None else running + weight
                    ladder = running if ladder is None else ladder + running
                for member in range(2):
                    place = quad * QUAD + 2 * pair + member
                    part = slice(member * PATCH, (member + 1) * PATCH)
                    plain[level, place] = running[:, part]
                    nested[level, place] = ladder[:, part]

    schedule(quads, cross_stage, half_stage, sums_stage)
    usage = usage_ref[...].astype(jnp.float32)
    moments = moments_ref[...]
    across = (((1,), (1,)), ((), ()))
    along_rows, along_cols = 0.0, 0.0
    for level in range(LEVELS):
        by_col, by_row = 0.0, 0.0
        for sublane in range(8):
            part = plain[level, :, sublane, :]
            by_col = by_col + part
            by_row = by_row + ((HALF + sublane) * part - 8.0 * nested[level, :, sublane, :])
        col_part = lax.dot_general(
            moments, by_col, across, precision=lax.Precision.HIGHEST, preferred_element_type=jnp.float32
        )
        row_part = lax.dot_general(
            moments, by_row, across, precision=lax.Precision.HIGHEST, preferred_element_type=jnp.float32
        )
        scale = usage[level : level + 1] / (col_part[0:1] + 1e-6)
        along_rows = along_rows + row_part[0:1] * scale
        along_cols = along_cols + col_part[1:2] * scale
    count = jnp.maximum(jnp.sum(usage, axis=0, keepdims=True), 1.0)
    return jnp.concatenate([along_rows, along_cols], axis=0) / count


def schedule(quads, cross_stage, half_stage, sums_stage):
    for turn in range(quads + 2):
        if turn >= 2:
            sums_stage(turn - 2, turn % 2)
        if 1 <= turn <= quads:
            half_stage((turn - 1) % 2)
        if turn < quads:
            cross_stage(turn, turn % 2)


def flow_kernel(*refs):
    ins, out_ref, scratch = refs[:9], refs[9], refs[10:]
    out_ref[...] = estimate(*ins, *scratch)


def combine_kernel(turn_ref, shared_ref, skip_ref, *outs):
    me = turn_ref[0]
    sections = shared_ref.shape[0]

    def mask_of(section):
        held = shared_ref[jnp.minimum(section, sections - 1), 2:3, :]
        return jnp.where(section < sections, held, jnp.zeros_like(held))

    def flow_of(section):
        return shared_ref[section, 0:2, :] * (mask_of(section) * mask_of(section + 1))

    flow_next = flow_of(me)
    outs[0][0] = flow_next
    outs[1][0] = skip_ref[...] * (mask_of(me) * mask_of(me + 2))
    outs[2][0] = lax.fori_loop(
        0, me, lambda section, held: held + flow_of(section), jnp.zeros_like(flow_next)
    ) + flow_next


def passed_along(block, axis, distance):
    devices = range(lax.axis_size(axis))
    route = [(i - distance, i) for i in devices if i - distance in devices]
    return lax.ppermute(block, axis, route)


def on_device(section_tile, placement, tissue_mask, level_use):
    window, forward, inverse_rows, inverse_cols, moments = tables()
    patches = placement.shape[0]
    side = section_tile.shape[1]
    tile = section_tile[0]
    sections = lax.axis_size("sec")
    vmem = pl.BlockSpec(memory_space=pltpu.VMEM)
    smem = pl.BlockSpec(memory_space=pltpu.SMEM)
    panels = pltpu.VMEM((side // PATCH, side, PATCH), jnp.float32)
    sums = pltpu.VMEM((LEVELS, patches, 8, PATCH), jnp.float32)
    params = pltpu.CompilerParams(vmem_limit_bytes=24 * 2**20)

    next_tile = passed_along(tile, "sec", -1)
    own_spec = pl.pallas_call(
        spectrum_kernel,
        out_shape=jax.ShapeDtypeStruct((patches // 2, PATCH, 2 * PATCH), jnp.bfloat16),
        in_specs=[smem, vmem, vmem, vmem],
        out_specs=vmem,
        scratch_shapes=[panels],
        compiler_params=params,
        cost_estimate=pl.CostEstimate(flops=4 * 10**9, bytes_accessed=3 * 2**20, transcendentals=0),
        name="own_spectrum",
    )(placement, tile, window, forward)
    skip_tile = passed_along(next_tile, "sec", -1)

    def flow(other_tile, name):
        return pl.pallas_call(
            flow_kernel,
            out_shape=jax.ShapeDtypeStruct((2, patches), jnp.float32),
            in_specs=[smem] + [vmem] * 8,
            out_specs=vmem,
            scratch_shapes=[
                panels,
                pltpu.VMEM((2, 2 * PATCH, 2 * PATCH), jnp.bfloat16),
                pltpu.VMEM((2, LEVELS * 2 * PATCH, 2 * PATCH), jnp.bfloat16),
                sums,
                sums,
            ],
            compiler_params=params,
            cost_estimate=pl.CostEstimate(flops=8 * 10**9, bytes_accessed=4 * 2**20, transcendentals=0),
            name=name,
        )(placement, other_tile, own_spec, level_use, window, forward, inverse_rows, inverse_cols, moments)

    flow_next = flow(next_tile, "flow_next")
    message = jnp.concatenate([flow_next, tissue_mask.astype(jnp.float32)], axis=0)
    shared = lax.all_to_all(jnp.broadcast_to(message, (sections,) + message.shape), "sec", 0, 0)
    flow_skip = flow(skip_tile, "flow_skip")
    turn = jnp.reshape(lax.axis_index("sec"), (1,)).astype(jnp.int32)
    out = jax.ShapeDtypeStruct((1, 2, patches), jnp.float32)
    return pl.pallas_call(
        combine_kernel,
        out_shape=(out, out, out),
        in_specs=[smem, vmem, vmem],
        out_specs=(vmem, vmem, vmem),
        name="combine",
    )(turn, shared, flow_skip)


def solution(mesh):
    in_specs = (
        P(("grp", "sec"), None, None),
        P("grp", None),
        P(("grp", "sec"), None),
        P(None, "grp"),
    )
    out_specs = (
        P(("grp", "sec"), None, None),
        P(("grp", "sec"), None, None),
        P(("grp", "sec"), None, None),
    )
    return jax.shard_map(
        on_device, mesh=mesh, in_specs=in_specs, out_specs=out_specs, check_vma=False
    )
```

```python
import functools

import jax
import jax.numpy as jnp
import numpy as np
from jax import lax
from jax.experimental import pallas as pl
from jax.experimental.pallas import tpu as pltpu
from jax.sharding import PartitionSpec as P

PATCH = 128
LEVELS = 3
HALF = PATCH // 2
PAIRS = 4
GROUP = 2 * PAIRS


def tables():
    index = np.arange(PATCH)
    angles = ((index[:, None] * index[None, :]) % PATCH).astype(np.float32) * np.float32(2.0 * np.pi / PATCH)
    cosine = np.cos(angles).astype(jnp.bfloat16).astype(np.float32)
    sine = (-np.sin(angles)).astype(jnp.bfloat16).astype(np.float32)
    signed = np.minimum(index, PATCH - index)
    bands = [(signed < PATCH // 2 ** (level + 1)).astype(np.float32) for level in range(LEVELS)]
    offset = np.where(index < HALF, index, index - PATCH).astype(np.float64)

    zero = np.zeros((PATCH, HALF), np.float32)
    cos_half, sin_half = cosine[:, :HALF], sine[:, :HALF]
    window = np.stack(
        [
            np.tile(np.concatenate(part, axis=1), (2, 1))
            for part in ([cos_half, zero], [sin_half, zero], [zero, cos_half], [zero, sin_half])
        ]
    )
    forward = np.concatenate([cosine, sine], axis=1) / PATCH

    def inverse_rows(level, kept, points):
        left = (cosine * bands[level])[points][:, kept], (sine * bands[level])[points][:, kept]
        return np.block([[left[0], left[1]], [-left[1], left[0]]])

    def inverse_cols(level, width, lanes, members, points):
        twice = np.where(np.arange(width) == 0, 1.0, 2.0)[:, None] * bands[level][:width, None] / PATCH
        table = np.zeros((2 * PATCH, 2 * PATCH), np.float32)
        for turn, patch in enumerate(members):
            group = lanes.index(patch) * width
            cols = slice(turn * len(points), (turn + 1) * len(points))
            table[group : group + width, cols] = cosine[:width][:, points] * twice
            table[PATCH + group : PATCH + group + width, cols] = sine[:width][:, points] * twice
        return table

    quarter, eighth = PATCH // 4, PATCH // 8
    kept = [index, np.r_[:quarter, PATCH - quarter : PATCH], np.r_[:eighth, PATCH - eighth : PATCH]]
    coarse = index[::2]
    rows = [
        inverse_rows(0, kept[0], index),
        inverse_rows(1, kept[1], index),
        inverse_rows(2, kept[2], coarse),
    ]
    by_eighth = [0, 4, 2, 6, 1, 5, 3, 7]
    cols = np.stack(
        [
            inverse_cols(0, HALF, [0, 1], [0, 1], index),
            inverse_cols(1, quarter, [0, 2, 1, 3], [0, 1], index),
            inverse_cols(1, quarter, [0, 2, 1, 3], [2, 3], index),
            inverse_cols(2, eighth, by_eighth, [0, 1, 2, 3], coarse),
            inverse_cols(2, eighth, by_eighth, [4, 5, 6, 7], coarse),
        ]
    )

    spectrum = np.fft.fft(offset)
    spectrum[np.minimum(index, PATCH - index) >= quarter] = 0.0
    smooth = 2.0 * np.real(np.fft.ifft(spectrum))[::2]
    moments = np.zeros((2, 8, PATCH), np.float32)
    moments[0, 0], moments[0, 1], moments[0, 2] = 1.0, offset, 1.0
    moments[1, 0], moments[1, 1], moments[1, 2] = 4.0, 2.0 * np.tile(smooth, 2), 2.0
    slopes = np.broadcast_to(smooth[:, None], (HALF, PATCH)).astype(np.float32)
    return (
        jnp.asarray(window),
        jnp.asarray(forward, jnp.bfloat16),
        *(jnp.asarray(table, jnp.bfloat16) for table in rows),
        jnp.asarray(cols, jnp.bfloat16),
        jnp.asarray(moments),
        jnp.asarray(slopes),
    )


def product(left, right):
    return jnp.dot(left, right, preferred_element_type=jnp.float32)


def fill_panels(tile_ref, panels):
    for panel in range(panels.shape[0]):
        panels[panel] = tile_ref[:, panel * PATCH : (panel + 1) * PATCH].astype(jnp.float32)


def pair_spectrum(pair, place_ref, panels, window_ref, forward):
    last = panels.shape[0] - 1
    lane = lax.broadcasted_iota(jnp.int32, (PATCH, PATCH), 1)
    turned, table = [], []
    for member in range(2):
        row = place_ref[0, 2 * pair + member]
        col = place_ref[1, 2 * pair + member]
        panel = lax.shift_right_logical(col, PATCH.bit_length() - 1)
        shift = col & (PATCH - 1)
        here = panels[panel, pl.ds(row, PATCH), :]
        beside = panels[jnp.minimum(panel + 1, last), pl.ds(row, PATCH), :]
        turned.append(jnp.where(lane >= shift, here, beside).astype(jnp.bfloat16))
        start = PATCH - shift
        table.append(
            jnp.concatenate(
                [
                    window_ref[2 * member, pl.ds(start, PATCH), :],
                    window_ref[2 * member + 1, pl.ds(start, PATCH), :],
                ],
                axis=1,
            ).astype(jnp.bfloat16)
        )
    cols = product(jnp.concatenate(turned, axis=1), jnp.concatenate(table, axis=0)).astype(jnp.bfloat16)
    crossed = jnp.concatenate([-cols[:, PATCH:], cols[:, :PATCH]], axis=1)
    return product(forward, jnp.concatenate([cols, crossed], axis=0)).astype(jnp.bfloat16)


def own_kernel(place_ref, tile_ref, window_ref, forward_ref, spec_ref, started_ref, panels):
    started_ref[...] = jnp.zeros_like(started_ref)
    fill_panels(tile_ref, panels)
    forward = forward_ref[...]
    for pair in range(spec_ref.shape[0]):
        spec_ref[pair] = pair_spectrum(pair, place_ref, panels, window_ref, forward)


def estimate(
    place_ref, tile_ref, spec_ref, usage_ref, window_ref, forward_ref, rows0_ref, rows1_ref, rows2_ref, cols_ref,
    moments_ref, slopes_ref, panels, cross0, cross1, cross2, half0, half1, half2, plain, nested,
):
    fill_panels(tile_ref, panels)
    groups = place_ref.shape[1] // GROUP
    quarter, eighth = PATCH // 4, PATCH // 8

    def packed(even, odd, width):
        lane = lax.broadcasted_iota(jnp.int32, even.shape, 1)
        return jnp.where((lane & (2 * width - 1)) < width, even, pltpu.roll(odd, width, 1))

    def cross_stage(group, slot):
        forward = forward_ref[...]
        inner = []
        for pair in range(PAIRS):
            place = group * PAIRS + pair
            other = pair_spectrum(place, place_ref, panels, window_ref, forward).astype(jnp.float32)
            own = spec_ref[place].astype(jnp.float32)
            own_real, own_imag = own[:, :PATCH], own[:, PATCH:]
            other_real, other_imag = other[:, :PATCH], other[:, PATCH:]
            real = own_real * other_real + own_imag * other_imag
            imag = own_imag * other_real - own_real * other_imag
            lanes = slice(pair % 2 * PATCH, (pair % 2 + 1) * PATCH)
            cross0[slot, pair // 2, :PATCH, lanes] = real.astype(jnp.bfloat16)
            cross0[slot, pair // 2, PATCH:, lanes] = imag.astype(jnp.bfloat16)
            inner.append(
                jnp.concatenate([real[:quarter], real[-quarter:], imag[:quarter], imag[-quarter:]], axis=0)
            )
        middle = [packed(inner[2 * turn], inner[2 * turn + 1], quarter) for turn in range(PAIRS // 2)]
        for turn in range(PAIRS // 2):
            cross1[slot, :, turn * PATCH : (turn + 1) * PATCH] = middle[turn].astype(jnp.bfloat16)
        inner = [
            jnp.concatenate(
                [part[:eighth], part[HALF - eighth : HALF], part[HALF : HALF + eighth], part[-eighth:]], axis=0
            )
            for part in middle
        ]
        cross2[slot] = packed(inner[0], inner[1], eighth).astype(jnp.bfloat16)

    def half_stage(slot):
        for turn in range(PAIRS // 2):
            half0[slot, turn] = product(rows0_ref[...], cross0[slot, turn]).astype(jnp.bfloat16)
        half1[slot] = product(rows1_ref[...], cross1[slot]).astype(jnp.bfloat16)
        half2[slot] = product(rows2_ref[...], cross2[slot]).astype(jnp.bfloat16)

    def lines(half, tile):
        lanes = slice(tile * PATCH, (tile + 1) * PATCH)
        middle = half.shape[0] // 2
        return jnp.concatenate([half[:middle, lanes], half[middle:, lanes]], axis=1)

    def keep_ladder(level, group, members, correl):
        running, ladder = None, None
        for turn in range(PATCH // 8):
            row = (turn * 8 + HALF) % PATCH
            block = correl[row : row + 8]
            weight = block * block
            running = weight if running is None else running + weight
            ladder = running if ladder is None else ladder + running
        for turn, member in enumerate(members):
            lanes = slice(turn * PATCH, (turn + 1) * PATCH)
            plain[level, group * GROUP + member] = running[:, lanes]
            nested[level, group * GROUP + member] = ladder[:, lanes]

    def sums_stage(group, slot):
        correl = product(
            jnp.concatenate([lines(half0.at[slot, pair // 2], pair % 2) for pair in range(PAIRS)], axis=0), cols_ref[0]
        )
        for pair in range(PAIRS):
            keep_ladder(0, group, (2 * pair, 2 * pair + 1), correl[pair * PATCH : (pair + 1) * PATCH])
        line = jnp.concatenate([lines(half1.at[slot], turn) for turn in range(PAIRS // 2)], axis=0)
        for part in range(2):
            correl = product(line, cols_ref[1 + part])
            for turn in range(PAIRS // 2):
                pair = 2 * turn + part
                keep_ladder(1, group, (2 * pair, 2 * pair + 1), correl[turn * PATCH : (turn + 1) * PATCH])
        line = lines(half2.at[slot], 0)
        for part in range(2):
            correl = product(line, cols_ref[3 + part])
            for turn in range(2):
                total, slope = None, None
                for row in range(0, HALF, 8):
                    block = correl[row : row + 8, turn * PATCH : (turn + 1) * PATCH]
                    weight = block * block
                    sloped = weight * slopes_ref[row : row + 8]
                    total = weight if total is None else total + weight
                    slope = sloped if slope is None else slope + sloped
                for member in range(2):
                    place = group * GROUP + 4 * part + 2 * turn + member
                    plain[2, place] = total
                    nested[2, place] = slope

    for turn in range(groups + 2):
        if turn >= 2:
            sums_stage(turn - 2, turn % 2)
        if 1 <= turn <= groups:
            half_stage((turn - 1) % 2)
        if turn < groups:
            cross_stage(turn, turn % 2)

    usage = usage_ref[...].astype(jnp.float32)
    across = (((1,), (1,)), ((), ()))
    shape = plain.shape[1], PATCH
    own_lanes = (lax.broadcasted_iota(jnp.int32, shape, 1) >= HALF) == (
        (lax.broadcasted_iota(jnp.int32, shape, 0) & 1) == 1
    )
    along_rows, along_cols = 0.0, 0.0
    for level in range(LEVELS):
        by_col, by_row = 0.0, 0.0
        for sublane in range(8):
            part = plain[level, :, sublane, :]
            by_col = by_col + part
            if level < 2:
                by_row = by_row + ((HALF + sublane) * part - 8.0 * nested[level, :, sublane, :])
            else:
                by_row = by_row + nested[level, :, sublane, :]
        if level == 2:
            by_col = jnp.where(own_lanes, by_col, 0.0)
            by_row = jnp.where(own_lanes, by_row, 0.0)
        col_part, row_part = (
            lax.dot_general(
                moments_ref[level // 2], part, across, precision=lax.Precision.HIGHEST,
                preferred_element_type=jnp.float32,
            )
            for part in (by_col, by_row)
        )
        scale = usage[level : level + 1] / (col_part[0:1] + 1e-6)
        along_rows = along_rows + row_part[2:3] * scale
        along_cols = along_cols + col_part[1:2] * scale
    count = jnp.maximum(jnp.sum(usage, axis=0, keepdims=True), 1.0)
    return jnp.concatenate([along_rows, along_cols], axis=0) / count


INS = 12


def next_kernel(*refs):
    ins, mask_ref, out_ref, scratch = refs[:INS], refs[INS], refs[INS + 1], refs[INS + 2 :]
    message = jnp.concatenate([estimate(*ins, *scratch), mask_ref[...].astype(jnp.float32)], axis=0)
    for section in range(out_ref.shape[0]):
        out_ref[section] = message


def skip_kernel(*refs):
    ins, out_ref, scratch = refs[:INS], refs[INS], refs[INS + 1 :]
    out_ref[...] = estimate(*ins, *scratch)


def combine_kernel(shared_ref, skip_ref, *outs):
    me = lax.axis_index("sec")
    sections = shared_ref.shape[0]

    def mask_of(section):
        held = shared_ref[jnp.minimum(section, sections - 1), 2:3, :]
        return jnp.where(section < sections, held, jnp.zeros_like(held))

    def flow_of(section):
        return shared_ref[section, 0:2, :] * (mask_of(section) * mask_of(section + 1))

    flow_next = flow_of(me)
    outs[0][0] = flow_next
    outs[1][0] = skip_ref[...] * (mask_of(me) * mask_of(me + 2))
    outs[2][0] = lax.fori_loop(
        0, me, lambda section, held: held + flow_of(section), jnp.zeros_like(flow_next)
    ) + flow_next


def passed_along(block, axis, distance):
    devices = range(lax.axis_size(axis))
    route = [(i - distance, i) for i in devices if i - distance in devices]
    return lax.ppermute(block, axis, route)


def on_device(section_tile, placement, tissue_mask, level_use):
    window, forward, *rest = tables()
    patches = placement.shape[0]
    side = section_tile.shape[1]
    tile = section_tile[0]
    sections = lax.axis_size("sec")
    vmem = pl.BlockSpec(memory_space=pltpu.VMEM)
    smem = pl.BlockSpec(memory_space=pltpu.SMEM)
    panels = pltpu.VMEM((side // PATCH, side, PATCH), jnp.float32)
    sums = pltpu.VMEM((LEVELS, patches, 8, PATCH), jnp.float32)
    corners = placement.T

    def limit(mebibytes):
        return pltpu.CompilerParams(vmem_limit_bytes=mebibytes * 2**20)

    next_tile = passed_along(tile, "sec", -1)
    own_spec, started = pl.pallas_call(
        own_kernel,
        out_shape=(
            jax.ShapeDtypeStruct((patches // 2, PATCH, 2 * PATCH), jnp.bfloat16),
            jax.ShapeDtypeStruct((8, PATCH), jnp.float32),
        ),
        in_specs=[smem, vmem, vmem, vmem],
        out_specs=(vmem, vmem),
        scratch_shapes=[panels],
        compiler_params=limit(8),
        cost_estimate=pl.CostEstimate(flops=4 * 10**9, bytes_accessed=3 * 2**20, transcendentals=0),
        name="own_spectrum",
    )(corners, tile, window, forward)
    later_tile, own_spec, _ = lax.optimization_barrier((tile, own_spec, started))
    skip_tile = passed_along(later_tile, "sec", -2)

    def flow(kernel, out_shape, other_tile, name, *more):
        return pl.pallas_call(
            kernel,
            out_shape=jax.ShapeDtypeStruct(out_shape, jnp.float32),
            in_specs=[smem] + [vmem] * (INS - 1 + len(more)),
            out_specs=vmem,
            scratch_shapes=[
                panels,
                pltpu.VMEM((2, PAIRS // 2, 2 * PATCH, 2 * PATCH), jnp.bfloat16),
                pltpu.VMEM((2, PATCH, 2 * PATCH), jnp.bfloat16),
                pltpu.VMEM((2, HALF, PATCH), jnp.bfloat16),
                pltpu.VMEM((2, PAIRS // 2, 2 * PATCH, 2 * PATCH), jnp.bfloat16),
                pltpu.VMEM((2, 2 * PATCH, 2 * PATCH), jnp.bfloat16),
                pltpu.VMEM((2, PATCH, PATCH), jnp.bfloat16),
                sums,
                sums,
            ],
            compiler_params=limit(12),
            cost_estimate=pl.CostEstimate(flops=8 * 10**9, bytes_accessed=4 * 2**20, transcendentals=0),
            name=name,
        )(corners, other_tile, own_spec, level_use, window, forward, *rest, *more)

    message = flow(next_kernel, (sections, 3, patches), next_tile, "flow_next", tissue_mask)
    shared = lax.all_to_all(message, "sec", 0, 0)
    flow_skip = flow(skip_kernel, (2, patches), skip_tile, "flow_skip")
    out = jax.ShapeDtypeStruct((1, 2, patches), jnp.float32)
    return pl.pallas_call(
        combine_kernel,
        out_shape=(out, out, out),
        in_specs=[vmem, vmem],
        out_specs=(vmem, vmem, vmem),
        compiler_params=limit(2),
        name="combine",
    )(shared, flow_skip)


def solution(mesh):
    in_specs = (
        P(("grp", "sec"), None, None),
        P("grp", None),
        P(("grp", "sec"), None),
        P(None, "grp"),
    )
    out_specs = (
        P(("grp", "sec"), None, None),
        P(("grp", "sec"), None, None),
        P(("grp", "sec"), None, None),
    )
    return jax.shard_map(
        on_device, mesh=mesh, in_specs=in_specs, out_specs=out_specs, check_vma=False
    )
```

```python
import functools

import jax
import jax.numpy as jnp
import numpy as np
from jax import lax
from jax.experimental import pallas as pl
from jax.experimental.pallas import tpu as pltpu
from jax.sharding import PartitionSpec as P


PATCH = 128
LEVELS = 3
HALF = PATCH // 2
PAIRS = 4
GROUP = 2 * PAIRS


def tables():
    index = np.arange(PATCH)
    angles = ((index[:, None] * index[None, :]) % PATCH).astype(np.float32) * np.float32(2.0 * np.pi / PATCH)
    cosine = np.cos(angles).astype(jnp.bfloat16).astype(np.float32)
    sine = (-np.sin(angles)).astype(jnp.bfloat16).astype(np.float32)
    signed = np.minimum(index, PATCH - index)
    bands = [(signed < PATCH // 2 ** (level + 1)).astype(np.float32) for level in range(LEVELS)]
    offset = np.where(index < HALF, index, index - PATCH).astype(np.float64)

    cos_half, sin_half = cosine[:, :HALF], sine[:, :HALF]
    forward = np.concatenate(
        [
            np.tile(np.concatenate(part, axis=1), (2, 1))
            for part in ([cos_half, sin_half], [sin_half, cos_half])
        ]
        + [cosine / PATCH, sine / PATCH]
    )

    def inverse_rows(level, kept, points):
        left = (cosine * bands[level])[points][:, kept], (sine * bands[level])[points][:, kept]
        return np.block([[left[0], left[1]], [-left[1], left[0]]])

    def inverse_cols(level, width, lanes, members, points):
        twice = np.where(np.arange(width) == 0, 1.0, 2.0)[:, None] * bands[level][:width, None] / PATCH
        table = np.zeros((2 * PATCH, 2 * PATCH), np.float32)
        for turn, patch in enumerate(members):
            group = lanes.index(patch) * width
            cols = slice(turn * len(points), (turn + 1) * len(points))
            table[group : group + width, cols] = cosine[:width][:, points] * twice
            table[PATCH + group : PATCH + group + width, cols] = sine[:width][:, points] * twice
        return table

    quarter, eighth = PATCH // 4, PATCH // 8
    kept = [index, np.r_[:quarter, PATCH - quarter : PATCH], np.r_[:eighth, PATCH - eighth : PATCH]]
    coarse = index[::2]
    rows = [
        inverse_rows(0, kept[0], index),
        inverse_rows(1, kept[1], index),
        inverse_rows(2, kept[2], coarse),
    ]
    by_eighth = [0, 4, 2, 6, 1, 5, 3, 7]
    cols = np.stack(
        [
            inverse_cols(0, HALF, [0, 1], [0, 1], index),
            inverse_cols(1, quarter, [0, 2, 1, 3], [0, 1], index),
            inverse_cols(1, quarter, [0, 2, 1, 3], [2, 3], index),
            inverse_cols(2, eighth, by_eighth, [0, 1, 2, 3], coarse),
            inverse_cols(2, eighth, by_eighth, [4, 5, 6, 7], coarse),
        ]
    )

    spectrum = np.fft.fft(offset)
    spectrum[np.minimum(index, PATCH - index) >= quarter] = 0.0
    smooth = 2.0 * np.real(np.fft.ifft(spectrum))[::2]
    moments = np.zeros((2, 8, PATCH), np.float32)
    moments[0, 0], moments[0, 1], moments[0, 2] = 1.0, offset, 1.0
    moments[1, 0], moments[1, 1], moments[1, 2] = 4.0, 2.0 * np.tile(smooth, 2), 2.0
    slopes = np.broadcast_to(smooth[:, None], (HALF, PATCH)).astype(np.float32)
    return (
        jnp.asarray(forward),
        *(jnp.asarray(table, jnp.bfloat16) for table in rows),
        jnp.asarray(cols, jnp.bfloat16),
        jnp.asarray(moments),
        jnp.asarray(slopes),
    )


def product(left, right):
    return jnp.dot(left, right, preferred_element_type=jnp.float32)


def fill_panels(tile_ref, panels):
    for panel in range(panels.shape[0]):
        panels[panel] = tile_ref[:, panel * PATCH : (panel + 1) * PATCH].astype(jnp.float32)


def transform_of(forward_ref):
    first = forward_ref.shape[0] - 2 * PATCH
    parts = [forward_ref[first + turn * PATCH : first + (turn + 1) * PATCH] for turn in range(2)]
    return jnp.concatenate(parts, axis=1).astype(jnp.bfloat16)


def pair_spectrum(pair, place_ref, panels, forward_ref, forward):
    last = panels.shape[0] - 1
    lane = lax.broadcasted_iota(jnp.int32, (PATCH, PATCH), 1)
    turned, table = [], []
    for member in range(2):
        row = place_ref[0, 2 * pair + member]
        col = place_ref[1, 2 * pair + member]
        panel = lax.shift_right_logical(col, PATCH.bit_length() - 1)
        shift = col & (PATCH - 1)
        here = panels[panel, pl.ds(row, PATCH), :]
        beside = panels[jnp.minimum(panel + 1, last), pl.ds(row, PATCH), :]
        turned.append(jnp.where(lane >= shift, here, beside).astype(jnp.bfloat16))
        mine = (lane >= HALF) == (member == 1)
        parts = [
            jnp.where(mine, forward_ref[pl.ds((2 * order + 1) * PATCH - shift, PATCH), :], 0.0)
            for order in (member, 1 - member)
        ]
        table.append(jnp.concatenate(parts, axis=1).astype(jnp.bfloat16))
    cols = product(jnp.concatenate(turned, axis=1), jnp.concatenate(table, axis=0)).astype(jnp.bfloat16)
    crossed = jnp.concatenate([-cols[:, PATCH:], cols[:, :PATCH]], axis=1)
    return product(forward, jnp.concatenate([cols, crossed], axis=0)).astype(jnp.bfloat16)


def with_corners(corners_ref, place_ref, sem, work):
    copy = pltpu.make_async_copy(corners_ref, place_ref, sem)
    copy.start()
    work()
    copy.wait()


def own_kernel(corners_ref, tile_ref, forward_ref, spec_ref, started_ref, held, panels, place_ref, sems):
    fetch = pltpu.make_async_copy(tile_ref, held, sems.at[0])
    fetch.start()
    started_ref[...] = jnp.zeros_like(started_ref)

    def fill():
        fetch.wait()
        fill_panels(held, panels)

    with_corners(corners_ref, place_ref, sems.at[1], fill)
    forward = transform_of(forward_ref)
    for pair in range(spec_ref.shape[0]):
        spec_ref[pair] = pair_spectrum(pair, place_ref, panels, forward_ref, forward)


def estimate(
    tile_refs, corners_ref, spec_ref, usage_ref, forward_ref, rows0_ref, rows1_ref, rows2_ref, cols_ref,
     moments_ref, slopes_ref, panels, place_ref, sem, cross0, cross1, cross2, half0, half1, half2, plain,
    nested,
):
    def fill():
        if len(tile_refs) == 1:
            fill_panels(tile_refs[0], panels)
        else:
            odd = lax.axis_index("sec") & 1
            for parity, tile_ref in enumerate(tile_refs):
                pl.when(odd == parity)(functools.partial(fill_panels, tile_ref, panels))

    with_corners(corners_ref, place_ref, sem, fill)
    groups = place_ref.shape[1] // GROUP
    quarter, eighth = PATCH // 4, PATCH // 8

    def packed(even, odd, width):
        lane = lax.broadcasted_iota(jnp.int32, even.shape, 1)
        return jnp.where((lane & (2 * width - 1)) < width, even, pltpu.roll(odd, width, 1))

    def cross_stage(group, slot):
        forward = transform_of(forward_ref)
        inner = []
        for pair in range(PAIRS):
            place = group * PAIRS + pair
            other = pair_spectrum(place, place_ref, panels, forward_ref, forward).astype(jnp.float32)
            own = spec_ref[place].astype(jnp.float32)
            own_real, own_imag = own[:, :PATCH], own[:, PATCH:]
            other_real, other_imag = other[:, :PATCH], other[:, PATCH:]
            real = own_real * other_real + own_imag * other_imag
            imag = own_imag * other_real - own_real * other_imag
            lanes = slice(pair % 2 * PATCH, (pair % 2 + 1) * PATCH)
            cross0[slot, pair // 2, :PATCH, lanes] = real.astype(jnp.bfloat16)
            cross0[slot, pair // 2, PATCH:, lanes] = imag.astype(jnp.bfloat16)
            inner.append(
                jnp.concatenate([real[:quarter], real[-quarter:], imag[:quarter], imag[-quarter:]], axis=0)
            )
        middle = [packed(inner[2 * turn], inner[2 * turn + 1], quarter) for turn in range(PAIRS // 2)]
        for turn in range(PAIRS // 2):
            cross1[slot, :, turn * PATCH : (turn + 1) * PATCH] = middle[turn].astype(jnp.bfloat16)
        inner = [
            jnp.concatenate(
                [part[:eighth], part[HALF - eighth : HALF], part[HALF : HALF + eighth], part[-eighth:]], axis=0
            )
            for part in middle
        ]
        cross2[slot] = packed(inner[0], inner[1], eighth).astype(jnp.bfloat16)

    def half_stage(slot):
        for turn in range(PAIRS // 2):
            half0[slot, turn] = product(rows0_ref[...], cross0[slot, turn]).astype(jnp.bfloat16)
        half1[slot] = product(rows1_ref[...], cross1[slot]).astype(jnp.bfloat16)
        half2[slot] = product(rows2_ref[...], cross2[slot]).astype(jnp.bfloat16)

    def lines(half, tile):
        lanes = slice(tile * PATCH, (tile + 1) * PATCH)
        middle = half.shape[0] // 2
        return jnp.concatenate([half[:middle, lanes], half[middle:, lanes]], axis=1)

    def keep_ladder(level, group, members, correl):
        running, ladder = None, None
        for turn in range(PATCH // 8):
            row = (turn * 8 + HALF) % PATCH
            block = correl[row : row + 8]
            weight = block * block
            running = weight if running is None else running + weight
            ladder = running if ladder is None else ladder + running
        for turn, member in enumerate(members):
            lanes = slice(turn * PATCH, (turn + 1) * PATCH)
            plain[level, group * GROUP + member] = running[:, lanes]
            nested[level, group * GROUP + member] = ladder[:, lanes]

    def sums_stage(group, slot):
        correl = product(
            jnp.concatenate([lines(half0.at[slot, pair // 2], pair % 2) for pair in range(PAIRS)], axis=0), cols_ref[0]
        )
        for pair in range(PAIRS):
            keep_ladder(0, group, (2 * pair, 2 * pair + 1), correl[pair * PATCH : (pair + 1) * PATCH])
        line = jnp.concatenate([lines(half1.at[slot], turn) for turn in range(PAIRS // 2)], axis=0)
        for part in range(2):
            correl = product(line, cols_ref[1 + part])
            for turn in range(PAIRS // 2):
                pair = 2 * turn + part
                keep_ladder(1, group, (2 * pair, 2 * pair + 1), correl[turn * PATCH : (turn + 1) * PATCH])
        line = lines(half2.at[slot], 0)
        for part in range(2):
            correl = product(line, cols_ref[3 + part])
            for turn in range(2):
                total, slope = None, None
                for row in range(0, HALF, 8):
                    block = correl[row : row + 8, turn * PATCH : (turn + 1) * PATCH]
                    weight = block * block
                    sloped = weight * slopes_ref[row : row + 8]
                    total = weight if total is None else total + weight
                    slope = sloped if slope is None else slope + sloped
                for member in range(2):
                    place = group * GROUP + 4 * part + 2 * turn + member
                    plain[2, place] = total
                    nested[2, place] = slope

    for turn in range(groups + 2):
        if turn < groups:
            cross_stage(turn, turn % 2)
        if 1 <= turn <= groups:
            half_stage((turn - 1) % 2)
        if turn >= 2:
            sums_stage(turn - 2, turn % 2)

    usage = usage_ref[...].astype(jnp.float32)
    across = (((1,), (1,)), ((), ()))
    shape = plain.shape[1], PATCH
    own_lanes = (lax.broadcasted_iota(jnp.int32, shape, 1) >= HALF) == (
        (lax.broadcasted_iota(jnp.int32, shape, 0) & 1) == 1
    )
    along_rows, along_cols = 0.0, 0.0
    for level in range(LEVELS):
        by_col, by_row = 0.0, 0.0
        for sublane in range(8):
            part = plain[level, :, sublane, :]
            by_col = by_col + part
            if level < 2:
                by_row = by_row + ((HALF + sublane) * part - 8.0 * nested[level, :, sublane, :])
            else:
                by_row = by_row + nested[level, :, sublane, :]
        if level == 2:
            by_col = jnp.where(own_lanes, by_col, 0.0)
            by_row = jnp.where(own_lanes, by_row, 0.0)
        col_part, row_part = (
            lax.dot_general(
                moments_ref[level // 2], part, across, precision=lax.Precision.HIGHEST,
                preferred_element_type=jnp.float32,
            )
            for part in (by_col, by_row)
        )
        scale = usage[level : level + 1] / (col_part[0:1] + 1e-6)
        along_rows = along_rows + row_part[2:3] * scale
        along_cols = along_cols + col_part[1:2] * scale
    count = jnp.maximum(jnp.sum(usage, axis=0, keepdims=True), 1.0)
    return jnp.concatenate([along_rows, along_cols], axis=0) / count


INS = 10


def next_kernel(*refs):
    ins, (tile_ref, mask_ref, out_ref), scratch = refs[:INS], refs[INS : INS + 3], refs[INS + 3 :]
    message = jnp.concatenate([estimate([tile_ref], *ins, *scratch), mask_ref[...].astype(jnp.float32)], axis=0)
    for section in range(out_ref.shape[0]):
        out_ref[section] = message


def skip_kernel(*refs):
    ins, tile_refs, out_ref, scratch = refs[:INS], refs[INS : INS + 2], refs[INS + 2], refs[INS + 3 :]
    out_ref[...] = estimate(tile_refs, *ins, *scratch)


def combine_kernel(shared_ref, skip_ref, *outs):
    me = lax.axis_index("sec")
    sections = shared_ref.shape[0]

    def mask_of(section):
        held = shared_ref[jnp.minimum(section, sections - 1), 2:3, :]
        return jnp.where(section < sections, held, jnp.zeros_like(held))

    def flow_of(section):
        return shared_ref[section, 0:2, :] * (mask_of(section) * mask_of(section + 1))

    flow_next = flow_of(me)
    outs[0][0] = flow_next
    outs[1][0] = skip_ref[...] * (mask_of(me) * mask_of(me + 2))
    outs[2][0] = lax.fori_loop(
        0, me, lambda section, held: held + flow_of(section), jnp.zeros_like(flow_next)
    ) + flow_next


def moved(block, axis, distance, receivers=(0, 1)):
    devices = range(lax.axis_size(axis))
    route = [(i + distance, i) for i in devices if i + distance in devices and i % 2 in receivers]
    return lax.ppermute(block, axis, route)


def on_device(section_tile, placement, tissue_mask, level_use):
    forward, *rest = tables()
    patches = placement.shape[0]
    side = section_tile.shape[1]
    tile = section_tile[0]
    sections = lax.axis_size("sec")
    vmem = pl.BlockSpec(memory_space=pltpu.VMEM)
    panels = (side // PATCH, side, PATCH)
    corners = placement.T
    corner_scratch = [pltpu.SMEM(corners.shape, corners.dtype), pltpu.SemaphoreType.DMA]
    spec = jax.ShapeDtypeStruct((patches // 2, PATCH, 2 * PATCH), jnp.bfloat16)
    sums = pltpu.VMEM((LEVELS, patches, 8, PATCH), jnp.float32)

    def limit(mebibytes):
        return pltpu.CompilerParams(vmem_limit_bytes=mebibytes * 2**20)

    next_tile = moved(tile, "sec", 1)
    even_tile = moved(tile, "sec", 2, (0,))
    own_spec, started = pl.pallas_call(
        own_kernel,
        out_shape=(spec, jax.ShapeDtypeStruct((8, PATCH), jnp.float32)),
        in_specs=[vmem, pl.BlockSpec(memory_space=pltpu.HBM), vmem],
        out_specs=(vmem, vmem),
        scratch_shapes=[
            pltpu.VMEM(tile.shape, tile.dtype),
            pltpu.VMEM(panels, jnp.float32),
            corner_scratch[0],
            pltpu.SemaphoreType.DMA((2,)),
        ],
        compiler_params=limit(8),
        cost_estimate=pl.CostEstimate(flops=4 * 10**9, bytes_accessed=3 * 2**20, transcendentals=0),
        name="own_spectrum",
    )(corners, tile, forward)
    later_tile, own_spec, _ = lax.optimization_barrier((tile, own_spec, started))
    odd_tile = moved(later_tile, "sec", 2, (1,))

    def flow(kernel, out_shape, *more):
        return pl.pallas_call(
            kernel,
            out_shape=jax.ShapeDtypeStruct(out_shape, jnp.float32),
            in_specs=[vmem] * (INS + len(more)),
            out_specs=vmem,
            scratch_shapes=[
                pltpu.VMEM(panels, jnp.float32),
                *corner_scratch,
                pltpu.VMEM((2, PAIRS // 2, 2 * PATCH, 2 * PATCH), jnp.bfloat16),
                pltpu.VMEM((2, PATCH, 2 * PATCH), jnp.bfloat16),
                pltpu.VMEM((2, HALF, PATCH), jnp.bfloat16),
                pltpu.VMEM((2, PAIRS // 2, 2 * PATCH, 2 * PATCH), jnp.bfloat16),
                pltpu.VMEM((2, 2 * PATCH, 2 * PATCH), jnp.bfloat16),
                pltpu.VMEM((2, PATCH, PATCH), jnp.bfloat16),
                sums,
                sums,
            ],
            compiler_params=limit(12),
            cost_estimate=pl.CostEstimate(flops=8 * 10**9, bytes_accessed=4 * 2**20, transcendentals=0),
        )(corners, own_spec, level_use, forward, *rest, *more)

    message = flow(next_kernel, (sections, 3, patches), next_tile, tissue_mask)
    shared = lax.all_to_all(message, "sec", 0, 0)
    flow_skip = flow(skip_kernel, (2, patches), even_tile, odd_tile)
    out = jax.ShapeDtypeStruct((1, 2, patches), jnp.float32)
    return pl.pallas_call(
        combine_kernel,
        out_shape=(out, out, out),
        in_specs=[vmem, vmem],
        out_specs=(vmem, vmem, vmem),
        compiler_params=limit(2),
        name="combine",
    )(shared, flow_skip)


def solution(mesh):
    in_specs = (
        P(("grp", "sec"), None, None),
        P("grp", None),
        P(("grp", "sec"), None),
        P(None, "grp"),
    )
    out_specs = (
        P(("grp", "sec"), None, None),
        P(("grp", "sec"), None, None),
        P(("grp", "sec"), None, None),
    )

    return jax.shard_map(on_device, mesh=mesh, in_specs=in_specs, out_specs=out_specs, check_vma=False)
```

```python
import functools

import jax
import jax.numpy as jnp
import numpy as np
from jax import lax
from jax.experimental import pallas as pl
from jax.experimental.pallas import tpu as pltpu
from jax.sharding import PartitionSpec as P


PATCH = 128
LEVELS = 3
HALF = PATCH // 2
PAIRS = 4
GROUP = 2 * PAIRS


def tables():
    index = np.arange(PATCH)
    angles = ((index[:, None] * index[None, :]) % PATCH).astype(np.float32) * np.float32(2.0 * np.pi / PATCH)
    cosine = np.cos(angles).astype(jnp.bfloat16).astype(np.float32)
    sine = (-np.sin(angles)).astype(jnp.bfloat16).astype(np.float32)
    signed = np.minimum(index, PATCH - index)
    bands = [(signed < PATCH // 2 ** (level + 1)).astype(np.float32) for level in range(LEVELS)]
    offset = np.where(index < HALF, index, index - PATCH).astype(np.float64)

    cos_half, sin_half = cosine[:, :HALF], sine[:, :HALF]
    forward = np.concatenate(
        [
            np.tile(np.concatenate(part, axis=1), (2, 1))
            for part in ([cos_half, sin_half], [sin_half, cos_half])
        ]
        + [cosine / PATCH, sine / PATCH]
    )

    def inverse_rows(level, kept, points):
        left = (cosine * bands[level])[points][:, kept], (sine * bands[level])[points][:, kept]
        return np.block([[left[0], left[1]], [-left[1], left[0]]])

    def inverse_cols(level, width, lanes, members, points):
        twice = np.where(np.arange(width) == 0, 1.0, 2.0)[:, None] * bands[level][:width, None] / PATCH
        table = np.zeros((2 * PATCH, 2 * PATCH), np.float32)
        for turn, patch in enumerate(members):
            group = lanes.index(patch) * width
            cols = slice(turn * len(points), (turn + 1) * len(points))
            table[group : group + width, cols] = cosine[:width][:, points] * twice
            table[PATCH + group : PATCH + group + width, cols] = sine[:width][:, points] * twice
        return table

    quarter, eighth = PATCH // 4, PATCH // 8
    kept = [index, np.r_[:quarter, PATCH - quarter : PATCH], np.r_[:eighth, PATCH - eighth : PATCH]]
    coarse = index[::2]
    rows = [
        inverse_rows(0, kept[0], index),
        inverse_rows(1, kept[1], index),
        inverse_rows(2, kept[2], coarse),
    ]
    by_eighth = [0, 4, 2, 6, 1, 5, 3, 7]
    cols = np.stack(
        [
            inverse_cols(0, HALF, [0, 1], [0, 1], index),
            inverse_cols(1, quarter, [0, 2, 1, 3], [0, 1], index),
            inverse_cols(1, quarter, [0, 2, 1, 3], [2, 3], index),
            inverse_cols(2, eighth, by_eighth, [0, 1, 2, 3], coarse),
            inverse_cols(2, eighth, by_eighth, [4, 5, 6, 7], coarse),
        ]
    )

    spectrum = np.fft.fft(offset)
    spectrum[np.minimum(index, PATCH - index) >= quarter] = 0.0
    smooth = 2.0 * np.real(np.fft.ifft(spectrum))[::2]
    moments = np.zeros((2, 8, PATCH), np.float32)
    moments[0, 0], moments[0, 1], moments[0, 2] = 1.0, offset, 1.0
    moments[1, 0], moments[1, 1], moments[1, 2] = 4.0, 2.0 * np.tile(smooth, 2), 2.0
    slopes = np.broadcast_to(smooth[:, None], (HALF, PATCH)).astype(np.float32)
    return (
        jnp.asarray(forward),
        *(jnp.asarray(table, jnp.bfloat16) for table in rows),
        jnp.asarray(cols, jnp.bfloat16),
        jnp.asarray(moments),
        jnp.asarray(slopes),
    )


def product(left, right):
    return jnp.dot(left, right, preferred_element_type=jnp.float32)


def fill_panels(tile_ref, panels):
    for panel in range(panels.shape[0]):
        panels[panel] = tile_ref[:, panel * PATCH : (panel + 1) * PATCH].astype(jnp.float32)


def transform_of(forward_ref):
    first = forward_ref.shape[0] - 2 * PATCH
    parts = [forward_ref[first + turn * PATCH : first + (turn + 1) * PATCH] for turn in range(2)]
    return jnp.concatenate(parts, axis=1).astype(jnp.bfloat16)


def pair_table(pair, place_ref, forward_ref):
    lane = lax.broadcasted_iota(jnp.int32, (PATCH, PATCH), 1)
    table = []
    for member in range(2):
        shift = place_ref[1, 2 * pair + member] & (PATCH - 1)
        mine = (lane >= HALF) == (member == 1)
        parts = [
            jnp.where(mine, forward_ref[pl.ds((2 * order + 1) * PATCH - shift, PATCH), :], 0.0)
            for order in (member, 1 - member)
        ]
        table.append(jnp.concatenate(parts, axis=1).astype(jnp.bfloat16))
    return jnp.concatenate(table, axis=0)


def pair_spectrum(pair, place_ref, panels, table, forward):
    last = panels.shape[0] - 1
    lane = lax.broadcasted_iota(jnp.int32, (PATCH, PATCH), 1)
    turned = []
    for member in range(2):
        row = place_ref[0, 2 * pair + member]
        col = place_ref[1, 2 * pair + member]
        panel = lax.shift_right_logical(col, PATCH.bit_length() - 1)
        here = panels[panel, pl.ds(row, PATCH), :]
        beside = panels[jnp.minimum(panel + 1, last), pl.ds(row, PATCH), :]
        turned.append(jnp.where(lane >= (col & (PATCH - 1)), here, beside).astype(jnp.bfloat16))
    cols = product(jnp.concatenate(turned, axis=1), table).astype(jnp.bfloat16)
    crossed = jnp.concatenate([-cols[:, PATCH:], cols[:, :PATCH]], axis=1)
    return product(forward, jnp.concatenate([cols, crossed], axis=0)).astype(jnp.bfloat16)


def with_corners(corners_ref, place_ref, sem, work):
    copy = pltpu.make_async_copy(corners_ref, place_ref, sem)
    copy.start()
    work()
    copy.wait()


def own_kernel(corners_ref, tile_ref, forward_ref, spec_ref, table_ref, held, panels, place_ref, sems):
    fetch = pltpu.make_async_copy(tile_ref, held, sems.at[0])
    fetch.start()

    def fill():
        fetch.wait()
        fill_panels(held, panels)

    with_corners(corners_ref, place_ref, sems.at[1], fill)
    forward = transform_of(forward_ref)
    for pair in range(spec_ref.shape[0]):
        table = pair_table(pair, place_ref, forward_ref)
        table_ref[pair] = table
        spec_ref[pair] = pair_spectrum(pair, place_ref, panels, table, forward)


def estimate(
    tile_refs, table_ref, corners_ref, spec_ref, usage_ref, forward_ref, rows0_ref, rows1_ref, rows2_ref, cols_ref,
     moments_ref, slopes_ref, panels, place_ref, sem, cross0, cross1, cross2, half0, half1, half2, plain,
    nested,
):
    def fill():
        if len(tile_refs) == 1:
            fill_panels(tile_refs[0], panels)
        else:
            odd = lax.axis_index("sec") & 1
            for parity, tile_ref in enumerate(tile_refs):
                pl.when(odd == parity)(functools.partial(fill_panels, tile_ref, panels))

    with_corners(corners_ref, place_ref, sem, fill)
    groups = place_ref.shape[1] // GROUP
    quarter, eighth = PATCH // 4, PATCH // 8

    def packed(even, odd, width):
        lane = lax.broadcasted_iota(jnp.int32, even.shape, 1)
        return jnp.where((lane & (2 * width - 1)) < width, even, pltpu.roll(odd, width, 1))

    def cross_stage(group, slot):
        forward = transform_of(forward_ref)
        inner = []
        for pair in range(PAIRS):
            place = group * PAIRS + pair
            table = pair_table(place, place_ref, forward_ref) if table_ref is None else table_ref[place]
            other = pair_spectrum(place, place_ref, panels, table, forward).astype(jnp.float32)
            own = spec_ref[place].astype(jnp.float32)
            own_real, own_imag = own[:, :PATCH], own[:, PATCH:]
            other_real, other_imag = other[:, :PATCH], other[:, PATCH:]
            real = own_real * other_real + own_imag * other_imag
            imag = own_imag * other_real - own_real * other_imag
            lanes = slice(pair % 2 * PATCH, (pair % 2 + 1) * PATCH)
            cross0[slot, pair // 2, :PATCH, lanes] = real.astype(jnp.bfloat16)
            cross0[slot, pair // 2, PATCH:, lanes] = imag.astype(jnp.bfloat16)
            inner.append(
                jnp.concatenate([real[:quarter], real[-quarter:], imag[:quarter], imag[-quarter:]], axis=0)
            )
        middle = [packed(inner[2 * turn], inner[2 * turn + 1], quarter) for turn in range(PAIRS // 2)]
        for turn in range(PAIRS // 2):
            cross1[slot, :, turn * PATCH : (turn + 1) * PATCH] = middle[turn].astype(jnp.bfloat16)
        inner = [
            jnp.concatenate(
                [part[:eighth], part[HALF - eighth : HALF], part[HALF : HALF + eighth], part[-eighth:]], axis=0
            )
            for part in middle
        ]
        cross2[slot] = packed(inner[0], inner[1], eighth).astype(jnp.bfloat16)

    def half_stage(slot):
        for turn in range(PAIRS // 2):
            half0[slot, turn] = product(rows0_ref[...], cross0[slot, turn]).astype(jnp.bfloat16)
        half1[slot] = product(rows1_ref[...], cross1[slot]).astype(jnp.bfloat16)
        half2[slot] = product(rows2_ref[...], cross2[slot]).astype(jnp.bfloat16)

    def lines(half, tile):
        lanes = slice(tile * PATCH, (tile + 1) * PATCH)
        middle = half.shape[0] // 2
        return jnp.concatenate([half[:middle, lanes], half[middle:, lanes]], axis=1)

    def keep_ladder(level, group, members, correl):
        running, ladder = None, None
        for turn in range(PATCH // 8):
            row = (turn * 8 + HALF) % PATCH
            block = correl[row : row + 8]
            weight = block * block
            running = weight if running is None else running + weight
            ladder = running if ladder is None else ladder + running
        sublane = lax.broadcasted_iota(jnp.int32, running.shape, 0).astype(jnp.float32)
        by_col = jnp.sum(running, axis=0, keepdims=True)
        by_row = jnp.sum((HALF + sublane) * running - 8.0 * ladder, axis=0, keepdims=True)
        for turn, member in enumerate(members):
            lanes = slice(turn * PATCH, (turn + 1) * PATCH)
            place = group * GROUP + member
            plain[level, place : place + 1] = by_col[:, lanes]
            nested[level, place : place + 1] = by_row[:, lanes]

    def sums_stage(group, slot):
        correl = product(
            jnp.concatenate([lines(half0.at[slot, pair // 2], pair % 2) for pair in range(PAIRS)], axis=0), cols_ref[0]
        )
        for pair in range(PAIRS):
            keep_ladder(0, group, (2 * pair, 2 * pair + 1), correl[pair * PATCH : (pair + 1) * PATCH])
        line = jnp.concatenate([lines(half1.at[slot], turn) for turn in range(PAIRS // 2)], axis=0)
        for part in range(2):
            correl = product(line, cols_ref[1 + part])
            for turn in range(PAIRS // 2):
                pair = 2 * turn + part
                keep_ladder(1, group, (2 * pair, 2 * pair + 1), correl[turn * PATCH : (turn + 1) * PATCH])
        line = lines(half2.at[slot], 0)
        for part in range(2):
            correl = product(line, cols_ref[3 + part])
            for turn in range(2):
                total, slope = None, None
                for row in range(0, HALF, 8):
                    block = correl[row : row + 8, turn * PATCH : (turn + 1) * PATCH]
                    weight = block * block
                    sloped = weight * slopes_ref[row : row + 8]
                    total = weight if total is None else total + weight
                    slope = sloped if slope is None else slope + sloped
                total = jnp.sum(total, axis=0, keepdims=True)
                slope = jnp.sum(slope, axis=0, keepdims=True)
                for member in range(2):
                    place = group * GROUP + 4 * part + 2 * turn + member
                    plain[2, place : place + 1] = total
                    nested[2, place : place + 1] = slope

    for turn in range(groups + 2):
        if turn < groups:
            cross_stage(turn, turn % 2)
        if 1 <= turn <= groups:
            half_stage((turn - 1) % 2)
        if turn >= 2:
            sums_stage(turn - 2, turn % 2)

    usage = usage_ref[...].astype(jnp.float32)
    across = (((1,), (1,)), ((), ()))
    shape = plain.shape[1], PATCH
    own_lanes = (lax.broadcasted_iota(jnp.int32, shape, 1) >= HALF) == (
        (lax.broadcasted_iota(jnp.int32, shape, 0) & 1) == 1
    )
    along_rows, along_cols = 0.0, 0.0
    for level in range(LEVELS):
        by_col, by_row = plain[level], nested[level]
        if level == 2:
            by_col = jnp.where(own_lanes, by_col, 0.0)
            by_row = jnp.where(own_lanes, by_row, 0.0)
        col_part, row_part = (
            lax.dot_general(
                moments_ref[level // 2], part, across, precision=lax.Precision.HIGHEST,
                preferred_element_type=jnp.float32,
            )
            for part in (by_col, by_row)
        )
        scale = usage[level : level + 1] / (col_part[0:1] + 1e-6)
        along_rows = along_rows + row_part[2:3] * scale
        along_cols = along_cols + col_part[1:2] * scale
    count = jnp.maximum(jnp.sum(usage, axis=0, keepdims=True), 1.0)
    return jnp.concatenate([along_rows, along_cols], axis=0) / count


INS = 10


def next_kernel(*refs):
    ins, (tile_ref, table_ref, mask_ref, out_ref), scratch = refs[:INS], refs[INS : INS + 4], refs[INS + 4 :]
    message = jnp.concatenate([estimate([tile_ref], table_ref, *ins, *scratch), mask_ref[...].astype(jnp.float32)], axis=0)
    for section in range(out_ref.shape[0]):
        out_ref[section] = message


def skip_kernel(*refs):
    ins, tile_refs, out_ref, scratch = refs[:INS], refs[INS : INS + 2], refs[INS + 2], refs[INS + 3 :]
    out_ref[...] = estimate(tile_refs, None, *ins, *scratch)


def combine_kernel(shared_ref, skip_ref, *outs):
    me = lax.axis_index("sec")
    sections = shared_ref.shape[0]

    def mask_of(section):
        held = shared_ref[jnp.minimum(section, sections - 1), 2:3, :]
        return jnp.where(section < sections, held, jnp.zeros_like(held))

    def flow_of(section):
        return shared_ref[section, 0:2, :] * (mask_of(section) * mask_of(section + 1))

    flow_next = flow_of(me)
    outs[0][0] = flow_next
    outs[1][0] = skip_ref[...] * (mask_of(me) * mask_of(me + 2))
    outs[2][0] = lax.fori_loop(
        0, me, lambda section, held: held + flow_of(section), jnp.zeros_like(flow_next)
    ) + flow_next


def moved(block, axis, distance, receivers=(0, 1)):
    devices = range(lax.axis_size(axis))
    route = [(i + distance, i) for i in devices if i + distance in devices and i % 2 in receivers]
    return lax.ppermute(block, axis, route)


def on_device(section_tile, placement, tissue_mask, level_use):
    forward, *rest = tables()
    patches = placement.shape[0]
    side = section_tile.shape[1]
    tile = section_tile[0]
    sections = lax.axis_size("sec")
    vmem = pl.BlockSpec(memory_space=pltpu.VMEM)
    panels = (side // PATCH, side, PATCH)
    corners = placement.T
    corner_scratch = [pltpu.SMEM(corners.shape, corners.dtype), pltpu.SemaphoreType.DMA]
    spec = jax.ShapeDtypeStruct((patches // 2, PATCH, 2 * PATCH), jnp.bfloat16)
    sums = pltpu.VMEM((LEVELS, patches, PATCH), jnp.float32)

    def limit(mebibytes):
        return pltpu.CompilerParams(vmem_limit_bytes=mebibytes * 2**20)

    next_tile = moved(tile, "sec", 1)
    even_tile = moved(tile, "sec", 2, (0,))
    own_spec, col_tables = pl.pallas_call(
        own_kernel,
        out_shape=(spec, jax.ShapeDtypeStruct((patches // 2, 2 * PATCH, 2 * PATCH), jnp.bfloat16)),
        in_specs=[vmem, pl.BlockSpec(memory_space=pltpu.HBM), vmem],
        out_specs=(vmem, vmem),
        scratch_shapes=[
            pltpu.VMEM(tile.shape, tile.dtype),
            pltpu.VMEM(panels, jnp.float32),
            corner_scratch[0],
            pltpu.SemaphoreType.DMA((2,)),
        ],
        compiler_params=limit(8),
        cost_estimate=pl.CostEstimate(flops=4 * 10**9, bytes_accessed=3 * 2**20, transcendentals=0),
        name="own_spectrum",
    )(corners, tile, forward)
    later_tile, own_spec = lax.optimization_barrier((tile, own_spec))
    odd_tile = moved(later_tile, "sec", 2, (1,))

    def flow(kernel, out_shape, *more):
        return pl.pallas_call(
            kernel,
            out_shape=jax.ShapeDtypeStruct(out_shape, jnp.float32),
            in_specs=[vmem] * (INS + len(more)),
            out_specs=vmem,
            scratch_shapes=[
                pltpu.VMEM(panels, jnp.float32),
                *corner_scratch,
                pltpu.VMEM((2, PAIRS // 2, 2 * PATCH, 2 * PATCH), jnp.bfloat16),
                pltpu.VMEM((2, PATCH, 2 * PATCH), jnp.bfloat16),
                pltpu.VMEM((2, HALF, PATCH), jnp.bfloat16),
                pltpu.VMEM((2, PAIRS // 2, 2 * PATCH, 2 * PATCH), jnp.bfloat16),
                pltpu.VMEM((2, 2 * PATCH, 2 * PATCH), jnp.bfloat16),
                pltpu.VMEM((2, PATCH, PATCH), jnp.bfloat16),
                sums,
                sums,
            ],
            compiler_params=limit(12),
            cost_estimate=pl.CostEstimate(flops=8 * 10**9, bytes_accessed=4 * 2**20, transcendentals=0),
        )(corners, own_spec, level_use, forward, *rest, *more)

    message = flow(next_kernel, (sections, 3, patches), next_tile, col_tables, tissue_mask)
    shared = lax.all_to_all(message, "sec", 0, 0)
    flow_skip = flow(skip_kernel, (2, patches), even_tile, odd_tile)
    out = jax.ShapeDtypeStruct((1, 2, patches), jnp.float32)
    return pl.pallas_call(
        combine_kernel,
        out_shape=(out, out, out),
        in_specs=[vmem, vmem],
        out_specs=(vmem, vmem, vmem),
        compiler_params=limit(2),
        name="combine",
    )(shared, flow_skip)


def solution(mesh):
    in_specs = (
        P(("grp", "sec"), None, None),
        P("grp", None),
        P(("grp", "sec"), None),
        P(None, "grp"),
    )
    out_specs = (
        P(("grp", "sec"), None, None),
        P(("grp", "sec"), None, None),
        P(("grp", "sec"), None, None),
    )

    return jax.shard_map(on_device, mesh=mesh, in_specs=in_specs, out_specs=out_specs, check_vma=False)
```

```python
import functools

import jax
import jax.numpy as jnp
import numpy as np
from jax import lax
from jax.experimental import pallas as pl
from jax.experimental.pallas import tpu as pltpu
from jax.sharding import PartitionSpec as P


PATCH = 128
LEVELS = 3
HALF = PATCH // 2
PAIRS = 4
GROUP = 2 * PAIRS


def tables():
    index = np.arange(PATCH)
    angles = ((index[:, None] * index[None, :]) % PATCH).astype(np.float32) * np.float32(2.0 * np.pi / PATCH)
    cosine = np.cos(angles).astype(jnp.bfloat16).astype(np.float32)
    sine = (-np.sin(angles)).astype(jnp.bfloat16).astype(np.float32)
    signed = np.minimum(index, PATCH - index)
    bands = [(signed < PATCH // 2 ** (level + 1)).astype(np.float32) for level in range(LEVELS)]
    offset = np.where(index < HALF, index, index - PATCH).astype(np.float64)

    cos_half, sin_half = cosine[:, :HALF], sine[:, :HALF]
    forward = np.concatenate(
        [
            np.tile(np.concatenate(part, axis=1), (2, 1))
            for part in ([cos_half, sin_half], [sin_half, cos_half])
        ]
        + [cosine / PATCH, sine / PATCH]
    )

    def inverse_rows(level, kept, points):
        left = (cosine * bands[level])[points][:, kept], (sine * bands[level])[points][:, kept]
        return np.block([[left[0], left[1]], [-left[1], left[0]]])

    def inverse_cols(level, width, lanes, members, points):
        twice = np.where(np.arange(width) == 0, 1.0, 2.0)[:, None] * bands[level][:width, None] / PATCH
        table = np.zeros((2 * PATCH, 2 * PATCH), np.float32)
        for turn, patch in enumerate(members):
            group = lanes.index(patch) * width
            cols = slice(turn * len(points), (turn + 1) * len(points))
            table[group : group + width, cols] = cosine[:width][:, points] * twice
            table[PATCH + group : PATCH + group + width, cols] = sine[:width][:, points] * twice
        return table

    quarter, eighth = PATCH // 4, PATCH // 8
    kept = [index, np.r_[:quarter, PATCH - quarter : PATCH], np.r_[:eighth, PATCH - eighth : PATCH]]
    coarse = index[::2]
    rows = [
        inverse_rows(0, kept[0], index),
        inverse_rows(1, kept[1], index),
        inverse_rows(2, kept[2], coarse),
    ]
    by_eighth = [0, 4, 2, 6, 1, 5, 3, 7]
    cols = np.stack(
        [
            inverse_cols(0, HALF, [0, 1], [0, 1], index),
            inverse_cols(1, quarter, [0, 2, 1, 3], [0, 1], index),
            inverse_cols(1, quarter, [0, 2, 1, 3], [2, 3], index),
            inverse_cols(2, eighth, by_eighth, [0, 1, 2, 3], coarse),
            inverse_cols(2, eighth, by_eighth, [4, 5, 6, 7], coarse),
        ]
    )

    spectrum = np.fft.fft(offset)
    spectrum[np.minimum(index, PATCH - index) >= quarter] = 0.0
    smooth = 2.0 * np.real(np.fft.ifft(spectrum))[::2]
    moments = np.zeros((2, 8, PATCH), np.float32)
    moments[0, 0], moments[0, 1], moments[0, 2] = 1.0, offset, 1.0
    moments[1, 0], moments[1, 1], moments[1, 2] = 4.0, 2.0 * np.tile(smooth, 2), 2.0
    slopes = np.broadcast_to(smooth[:, None], (HALF, PATCH)).astype(np.float32)
    return (
        jnp.asarray(forward),
        *(jnp.asarray(table, jnp.bfloat16) for table in rows),
        jnp.asarray(cols, jnp.bfloat16),
        jnp.asarray(moments),
        jnp.asarray(slopes),
    )


def product(left, right):
    return jnp.dot(left, right, preferred_element_type=jnp.float32)


def fill_panels(tile_ref, panels):
    for panel in range(panels.shape[0]):
        panels[panel] = tile_ref[:, panel * PATCH : (panel + 1) * PATCH].astype(jnp.float32)


def transform_of(forward_ref):
    first = forward_ref.shape[0] - 2 * PATCH
    parts = [forward_ref[first + turn * PATCH : first + (turn + 1) * PATCH] for turn in range(2)]
    return jnp.concatenate(parts, axis=1).astype(jnp.bfloat16)


class Direct:
    def __init__(self, corners_ref):
        self.values = corners_ref[...]

    def __getitem__(self, at):
        return self.values[at[0], at[1]]


def pair_table(pair, place_ref, forward_ref):
    lane = lax.broadcasted_iota(jnp.int32, (PATCH, PATCH), 1)
    table = []
    for member in range(2):
        shift = place_ref[1, 2 * pair + member] & (PATCH - 1)
        mine = (lane >= HALF) == (member == 1)
        parts = [
            jnp.where(mine, forward_ref[pl.ds((2 * order + 1) * PATCH - shift, PATCH), :], 0.0)
            for order in (member, 1 - member)
        ]
        table.append(jnp.concatenate(parts, axis=1).astype(jnp.bfloat16))
    return jnp.concatenate(table, axis=0)


def turned_patches(pair, place_ref, panels):
    last = panels.shape[0] - 1
    lane = lax.broadcasted_iota(jnp.int32, (PATCH, PATCH), 1)
    turned = []
    for member in range(2):
        row = place_ref[0, 2 * pair + member]
        col = place_ref[1, 2 * pair + member]
        panel = lax.shift_right_logical(col, PATCH.bit_length() - 1)
        here = panels[panel, pl.ds(row, PATCH), :]
        beside = panels[jnp.minimum(panel + 1, last), pl.ds(row, PATCH), :]
        turned.append(jnp.where(lane >= (col & (PATCH - 1)), here, beside).astype(jnp.bfloat16))
    return jnp.concatenate(turned, axis=1)


def crossed(parts):
    return jnp.concatenate([-parts[:, PATCH:], parts[:, :PATCH]], axis=1)


def spectrum_by_columns(patches, table, forward):
    cols = product(patches, table).astype(jnp.bfloat16)
    return product(forward, jnp.concatenate([cols, crossed(cols)], axis=0)).astype(jnp.bfloat16)


def spectrum_by_rows(patches, table, stacked):
    rows = product(stacked, patches).astype(jnp.bfloat16)
    return (product(rows[:PATCH], table) + product(rows[PATCH:], crossed(table))).astype(jnp.bfloat16)


def own_kernel(corners_ref, tile_ref, tables_ref, spec_ref, table_ref, held, panels, forward_ref, corners, sems):
    copies = [
        pltpu.make_async_copy(source, target, sems.at[turn])
        for turn, (source, target) in enumerate(((tile_ref, held), (tables_ref, forward_ref), (corners_ref, corners)))
    ]
    for copy in copies:
        copy.start()
    for copy in copies:
        copy.wait()
    place_ref = Direct(corners)
    stacked = forward_ref[forward_ref.shape[0] - 2 * PATCH :].astype(jnp.bfloat16)
    fill_panels(held, panels)
    for pair in range(spec_ref.shape[0]):
        table = pair_table(pair, place_ref, forward_ref)
        table_ref[pair] = table
        spec_ref[pair] = spectrum_by_rows(turned_patches(pair, place_ref, panels), table, stacked)


def estimate(
    tile_refs, table_ref, corners_ref, spec_ref, usage_ref, forward_ref, rows0_ref, rows1_ref, rows2_ref, cols_ref,
     moments_ref, slopes_ref, panels, cross0, cross1, cross2, half0, half1, half2, plain,
    nested,
):
    def fill():
        if len(tile_refs) == 1:
            fill_panels(tile_refs[0], panels)
        else:
            odd = lax.axis_index("sec") & 1
            for parity, tile_ref in enumerate(tile_refs):
                pl.when(odd == parity)(functools.partial(fill_panels, tile_ref, panels))

    fill()
    groups = corners_ref.shape[1] // GROUP
    place_ref = Direct(corners_ref)
    quarter, eighth = PATCH // 4, PATCH // 8

    def packed(even, odd, width):
        lane = lax.broadcasted_iota(jnp.int32, even.shape, 1)
        return jnp.where((lane & (2 * width - 1)) < width, even, pltpu.roll(odd, width, 1))

    def cross_stage(group, slot):
        forward = transform_of(forward_ref)
        inner = []
        for pair in range(PAIRS):
            place = group * PAIRS + pair
            table = pair_table(place, place_ref, forward_ref) if table_ref is None else table_ref[place]
            other = spectrum_by_columns(turned_patches(place, place_ref, panels), table, forward).astype(jnp.float32)
            own = spec_ref[place].astype(jnp.float32)
            own_real, own_imag = own[:, :PATCH], own[:, PATCH:]
            other_real, other_imag = other[:, :PATCH], other[:, PATCH:]
            real = own_real * other_real + own_imag * other_imag
            imag = own_imag * other_real - own_real * other_imag
            lanes = slice(pair % 2 * PATCH, (pair % 2 + 1) * PATCH)
            cross0[slot, pair // 2, :PATCH, lanes] = real.astype(jnp.bfloat16)
            cross0[slot, pair // 2, PATCH:, lanes] = imag.astype(jnp.bfloat16)
            inner.append(
                jnp.concatenate([real[:quarter], real[-quarter:], imag[:quarter], imag[-quarter:]], axis=0)
            )
        middle = [packed(inner[2 * turn], inner[2 * turn + 1], quarter) for turn in range(PAIRS // 2)]
        for turn in range(PAIRS // 2):
            cross1[slot, :, turn * PATCH : (turn + 1) * PATCH] = middle[turn].astype(jnp.bfloat16)
        inner = [
            jnp.concatenate(
                [part[:eighth], part[HALF - eighth : HALF], part[HALF : HALF + eighth], part[-eighth:]], axis=0
            )
            for part in middle
        ]
        cross2[slot] = packed(inner[0], inner[1], eighth).astype(jnp.bfloat16)

    def half_stage(source, slot):
        for turn in range(PAIRS // 2):
            half0[slot, turn] = product(rows0_ref[...], cross0[source, turn]).astype(jnp.bfloat16)
        half1[slot] = product(rows1_ref[...], cross1[source]).astype(jnp.bfloat16)
        half2[slot] = product(rows2_ref[...], cross2[source]).astype(jnp.bfloat16)

    def lines(half, tile):
        lanes = slice(tile * PATCH, (tile + 1) * PATCH)
        middle = half.shape[0] // 2
        return jnp.concatenate([half[:middle, lanes], half[middle:, lanes]], axis=1)

    def keep_ladder(level, group, members, correl):
        running, ladder = None, None
        for turn in range(PATCH // 8):
            row = (turn * 8 + HALF) % PATCH
            block = correl[row : row + 8]
            weight = block * block
            running = weight if running is None else running + weight
            ladder = running if ladder is None else ladder + running
        sublane = lax.broadcasted_iota(jnp.int32, running.shape, 0).astype(jnp.float32)
        by_col = jnp.sum(running, axis=0, keepdims=True)
        by_row = jnp.sum((HALF + sublane) * running - 8.0 * ladder, axis=0, keepdims=True)
        for turn, member in enumerate(members):
            lanes = slice(turn * PATCH, (turn + 1) * PATCH)
            place = group * GROUP + member
            plain[level, place : place + 1] = by_col[:, lanes]
            nested[level, place : place + 1] = by_row[:, lanes]

    def sums_stage(group, slot):
        correl = product(
            jnp.concatenate([lines(half0.at[slot, pair // 2], pair % 2) for pair in range(PAIRS)], axis=0), cols_ref[0]
        )
        for pair in range(PAIRS):
            keep_ladder(0, group, (2 * pair, 2 * pair + 1), correl[pair * PATCH : (pair + 1) * PATCH])
        line = jnp.concatenate([lines(half1.at[slot], turn) for turn in range(PAIRS // 2)], axis=0)
        for part in range(2):
            correl = product(line, cols_ref[1 + part])
            for turn in range(PAIRS // 2):
                pair = 2 * turn + part
                keep_ladder(1, group, (2 * pair, 2 * pair + 1), correl[turn * PATCH : (turn + 1) * PATCH])
        line = lines(half2.at[slot], 0)
        for part in range(2):
            correl = product(line, cols_ref[3 + part])
            for turn in range(2):
                total, slope = None, None
                for row in range(0, HALF, 8):
                    block = correl[row : row + 8, turn * PATCH : (turn + 1) * PATCH]
                    weight = block * block
                    sloped = weight * slopes_ref[row : row + 8]
                    total = weight if total is None else total + weight
                    slope = sloped if slope is None else slope + sloped
                total = jnp.sum(total, axis=0, keepdims=True)
                slope = jnp.sum(slope, axis=0, keepdims=True)
                for member in range(2):
                    place = group * GROUP + 4 * part + 2 * turn + member
                    plain[2, place : place + 1] = total
                    nested[2, place : place + 1] = slope

    for turn in range(groups + 4):
        if turn < groups:
            cross_stage(turn, turn % 4)
        if 3 <= turn <= groups + 2:
            half_stage((turn - 3) % 4, (turn - 1) % 2)
        if turn >= 4:
            sums_stage(turn - 4, turn % 2)

    usage = usage_ref[...].astype(jnp.float32)
    across = (((1,), (1,)), ((), ()))
    shape = plain.shape[1], PATCH
    own_lanes = (lax.broadcasted_iota(jnp.int32, shape, 1) >= HALF) == (
        (lax.broadcasted_iota(jnp.int32, shape, 0) & 1) == 1
    )
    along_rows, along_cols = 0.0, 0.0
    for level in range(LEVELS):
        by_col, by_row = plain[level], nested[level]
        if level == 2:
            by_col = jnp.where(own_lanes, by_col, 0.0)
            by_row = jnp.where(own_lanes, by_row, 0.0)
        col_part, row_part = (
            lax.dot_general(
                moments_ref[level // 2], part, across, precision=lax.Precision.HIGHEST,
                preferred_element_type=jnp.float32,
            )
            for part in (by_col, by_row)
        )
        scale = usage[level : level + 1] / (col_part[0:1] + 1e-6)
        along_rows = along_rows + row_part[2:3] * scale
        along_cols = along_cols + col_part[1:2] * scale
    count = jnp.maximum(jnp.sum(usage, axis=0, keepdims=True), 1.0)
    return jnp.concatenate([along_rows, along_cols], axis=0) / count


INS = 10


def next_kernel(*refs):
    ins, (tile_ref, table_ref, mask_ref, out_ref), scratch = refs[:INS], refs[INS : INS + 4], refs[INS + 4 :]
    message = jnp.concatenate([estimate([tile_ref], table_ref, *ins, *scratch), mask_ref[...].astype(jnp.float32)], axis=0)
    for section in range(out_ref.shape[0]):
        out_ref[section] = message


def skip_kernel(*refs):
    ins, tile_refs, out_ref, scratch = refs[:INS], refs[INS : INS + 2], refs[INS + 2], refs[INS + 3 :]
    out_ref[...] = estimate(tile_refs, None, *ins, *scratch)


def combine_kernel(shared_ref, skip_ref, *outs):
    me = lax.axis_index("sec")
    sections = shared_ref.shape[0]

    def mask_of(section):
        held = shared_ref[jnp.minimum(section, sections - 1), 2:3, :]
        return jnp.where(section < sections, held, jnp.zeros_like(held))

    def flow_of(section):
        return shared_ref[section, 0:2, :] * (mask_of(section) * mask_of(section + 1))

    flow_next = flow_of(me)
    outs[0][0] = flow_next
    outs[1][0] = skip_ref[...] * (mask_of(me) * mask_of(me + 2))
    outs[2][0] = lax.fori_loop(
        0, me, lambda section, held: held + flow_of(section), jnp.zeros_like(flow_next)
    ) + flow_next


def moved(block, axis, distance, receivers=(0, 1)):
    devices = range(lax.axis_size(axis))
    route = [(i + distance, i) for i in devices if i + distance in devices and i % 2 in receivers]
    return lax.ppermute(block, axis, route)


def on_device(section_tile, placement, tissue_mask, level_use):
    forward, *rest = tables()
    patches = placement.shape[0]
    side = section_tile.shape[1]
    tile = section_tile[0]
    sections = lax.axis_size("sec")
    vmem = pl.BlockSpec(memory_space=pltpu.VMEM)
    panels = (side // PATCH, side, PATCH)
    corners = placement.T
    spec = jax.ShapeDtypeStruct((patches // 2, PATCH, 2 * PATCH), jnp.bfloat16)
    sums = pltpu.VMEM((LEVELS, patches, PATCH), jnp.float32)

    def limit(mebibytes):
        return pltpu.CompilerParams(vmem_limit_bytes=mebibytes * 2**20)

    next_tile = moved(tile, "sec", 1)
    even_tile = moved(tile, "sec", 2, (0,))
    own_spec, col_tables = pl.pallas_call(
        own_kernel,
        out_shape=(spec, jax.ShapeDtypeStruct((patches // 2, 2 * PATCH, 2 * PATCH), jnp.bfloat16)),
        in_specs=[pl.BlockSpec(memory_space=pltpu.HBM)] * 3,
        out_specs=(vmem, vmem),
        scratch_shapes=[
            pltpu.VMEM(tile.shape, tile.dtype),
            pltpu.VMEM(panels, jnp.float32),
            pltpu.VMEM(forward.shape, forward.dtype),
            pltpu.VMEM(corners.shape, corners.dtype),
            pltpu.SemaphoreType.DMA((3,)),
        ],
        compiler_params=limit(8),
        cost_estimate=pl.CostEstimate(flops=4 * 10**9, bytes_accessed=3 * 2**20, transcendentals=0),
        name="own_spectrum",
    )(*(pltpu.with_memory_space_constraint(array, pltpu.HBM) for array in (corners, tile, forward)))
    later_tile, own_spec = lax.optimization_barrier((tile, own_spec))
    odd_tile = moved(later_tile, "sec", 2, (1,))

    def flow(kernel, out_shape, *more):
        return pl.pallas_call(
            kernel,
            out_shape=jax.ShapeDtypeStruct(out_shape, jnp.float32),
            in_specs=[vmem] * (INS + len(more)),
            out_specs=vmem,
            scratch_shapes=[
                pltpu.VMEM(panels, jnp.float32),
                pltpu.VMEM((4, PAIRS // 2, 2 * PATCH, 2 * PATCH), jnp.bfloat16),
                pltpu.VMEM((4, PATCH, 2 * PATCH), jnp.bfloat16),
                pltpu.VMEM((4, HALF, PATCH), jnp.bfloat16),
                pltpu.VMEM((2, PAIRS // 2, 2 * PATCH, 2 * PATCH), jnp.bfloat16),
                pltpu.VMEM((2, 2 * PATCH, 2 * PATCH), jnp.bfloat16),
                pltpu.VMEM((2, PATCH, PATCH), jnp.bfloat16),
                sums,
                sums,
            ],
            compiler_params=limit(12),
            cost_estimate=pl.CostEstimate(flops=8 * 10**9, bytes_accessed=4 * 2**20, transcendentals=0),
        )(corners, own_spec, level_use, forward, *rest, *more)

    message = flow(next_kernel, (sections, 3, patches), next_tile, col_tables, tissue_mask)
    shared = lax.all_to_all(message, "sec", 0, 0)
    flow_skip = flow(skip_kernel, (2, patches), even_tile, odd_tile)
    out = jax.ShapeDtypeStruct((1, 2, patches), jnp.float32)
    return pl.pallas_call(
        combine_kernel,
        out_shape=(out, out, out),
        in_specs=[vmem, vmem],
        out_specs=(vmem, vmem, vmem),
        compiler_params=limit(2),
        name="combine",
    )(shared, flow_skip)


def solution(mesh):
    in_specs = (
        P(("grp", "sec"), None, None),
        P("grp", None),
        P(("grp", "sec"), None),
        P(None, "grp"),
    )
    out_specs = (
        P(("grp", "sec"), None, None),
        P(("grp", "sec"), None, None),
        P(("grp", "sec"), None, None),
    )

    return jax.shard_map(on_device, mesh=mesh, in_specs=in_specs, out_specs=out_specs, check_vma=False)
```

```python
import functools

import jax
import jax.numpy as jnp
import numpy as np
from jax import lax
from jax.experimental import pallas as pl
from jax.experimental.pallas import tpu as pltpu
from jax.sharding import PartitionSpec as P


PATCH = 128
LEVELS = 3
HALF = PATCH // 2
PAIRS = 4
GROUP = 2 * PAIRS


def tables():
    index = np.arange(PATCH)
    angles = ((index[:, None] * index[None, :]) % PATCH).astype(np.float32) * np.float32(2.0 * np.pi / PATCH)
    cosine = np.cos(angles).astype(jnp.bfloat16).astype(np.float32)
    sine = (-np.sin(angles)).astype(jnp.bfloat16).astype(np.float32)
    signed = np.minimum(index, PATCH - index)
    bands = [(signed < PATCH // 2 ** (level + 1)).astype(np.float32) for level in range(LEVELS)]
    offset = np.where(index < HALF, index, index - PATCH).astype(np.float64)

    cos_half, sin_half = cosine[:, :HALF], sine[:, :HALF]
    forward = np.concatenate(
        [
            np.tile(np.concatenate(part, axis=1), (2, 1))
            for part in ([cos_half, sin_half], [sin_half, cos_half])
        ]
        + [cosine / PATCH, sine / PATCH]
    )

    def inverse_rows(level, kept, points):
        left = (cosine * bands[level])[points][:, kept], (sine * bands[level])[points][:, kept]
        return np.block([[left[0], left[1]], [-left[1], left[0]]])

    def inverse_cols(level, width, lanes, members, points):
        twice = np.where(np.arange(width) == 0, 1.0, 2.0)[:, None] * bands[level][:width, None] / PATCH
        table = np.zeros((2 * PATCH, 2 * PATCH), np.float32)
        for turn, patch in enumerate(members):
            group = lanes.index(patch) * width
            cols = slice(turn * len(points), (turn + 1) * len(points))
            table[group : group + width, cols] = cosine[:width][:, points] * twice
            table[PATCH + group : PATCH + group + width, cols] = sine[:width][:, points] * twice
        return table

    quarter, eighth = PATCH // 4, PATCH // 8
    kept = [index, np.r_[:quarter, PATCH - quarter : PATCH], np.r_[:eighth, PATCH - eighth : PATCH]]
    coarse = index[::2]
    rows = [
        inverse_rows(0, kept[0], index),
        inverse_rows(1, kept[1], index),
        inverse_rows(2, kept[2], coarse),
    ]
    by_eighth = [0, 4, 2, 6, 1, 5, 3, 7]
    cols = np.stack(
        [
            inverse_cols(0, HALF, [0, 1], [0, 1], index),
            inverse_cols(1, quarter, [0, 2, 1, 3], [0, 1], index),
            inverse_cols(1, quarter, [0, 2, 1, 3], [2, 3], index),
            inverse_cols(2, eighth, by_eighth, [0, 1, 2, 3], coarse),
            inverse_cols(2, eighth, by_eighth, [4, 5, 6, 7], coarse),
        ]
    )

    spectrum = np.fft.fft(offset)
    spectrum[np.minimum(index, PATCH - index) >= quarter] = 0.0
    smooth = 2.0 * np.real(np.fft.ifft(spectrum))[::2]
    moments = np.zeros((2, 8, PATCH), np.float32)
    moments[0, 0], moments[0, 1], moments[0, 2] = 1.0, offset, 1.0
    moments[1, 0], moments[1, 1], moments[1, 2] = 4.0, 2.0 * np.tile(smooth, 2), 2.0
    slopes = np.broadcast_to(smooth[:, None], (HALF, PATCH)).astype(np.float32)
    return (
        jnp.asarray(forward),
        *(jnp.asarray(table, jnp.bfloat16) for table in rows),
        jnp.asarray(cols, jnp.bfloat16),
        jnp.asarray(moments),
        jnp.asarray(slopes),
    )


def product(left, right):
    return jnp.dot(left, right, preferred_element_type=jnp.float32)


def fill_panels(tile_ref, panels):
    for panel in range(panels.shape[0]):
        panels[panel] = tile_ref[:, panel * PATCH : (panel + 1) * PATCH].astype(jnp.float32)


def stacked_of(forward_ref):
    return forward_ref[forward_ref.shape[0] - 2 * PATCH :].astype(jnp.bfloat16)


class Direct:
    def __init__(self, corners_ref):
        self.values = corners_ref[...]

    def __getitem__(self, at):
        return self.values[at[0], at[1]]


def pair_table(pair, place_ref, forward_ref):
    lane = lax.broadcasted_iota(jnp.int32, (PATCH, PATCH), 1)
    table = []
    for member in range(2):
        shift = place_ref[1, 2 * pair + member] & (PATCH - 1)
        mine = (lane >= HALF) == (member == 1)
        parts = [
            jnp.where(mine, forward_ref[pl.ds((2 * order + 1) * PATCH - shift, PATCH), :], 0.0)
            for order in (member, 1 - member)
        ]
        table.append(jnp.concatenate(parts, axis=1).astype(jnp.bfloat16))
    table = jnp.concatenate(table, axis=0)
    return table, crossed(table)


def turned_patches(pair, place_ref, panels):
    last = panels.shape[0] - 1
    lane = lax.broadcasted_iota(jnp.int32, (PATCH, PATCH), 1)
    turned = []
    for member in range(2):
        row = place_ref[0, 2 * pair + member]
        col = place_ref[1, 2 * pair + member]
        panel = lax.shift_right_logical(col, PATCH.bit_length() - 1)
        here = panels[panel, pl.ds(row, PATCH), :]
        beside = panels[jnp.minimum(panel + 1, last), pl.ds(row, PATCH), :]
        turned.append(jnp.where(lane >= (col & (PATCH - 1)), here, beside).astype(jnp.bfloat16))
    return jnp.concatenate(turned, axis=1)


def crossed(parts):
    return jnp.concatenate([-parts[:, PATCH:], parts[:, :PATCH]], axis=1)


def spectrum_of(patches, table, stacked):
    rows = product(stacked, patches).astype(jnp.bfloat16)
    return (product(rows[:PATCH], table[0]) + product(rows[PATCH:], table[1])).astype(jnp.bfloat16)


def own_kernel(corners_ref, tile_ref, tables_ref, spec_ref, wide_ref, table_ref, held, panels, forward_ref, corners, sems):
    copies = [
        pltpu.make_async_copy(source, target, sems.at[turn])
        for turn, (source, target) in enumerate(((tile_ref, held), (tables_ref, forward_ref), (corners_ref, corners)))
    ]
    for copy in copies:
        copy.start()
    for copy in copies:
        copy.wait()
    place_ref = Direct(corners)
    stacked = stacked_of(forward_ref)
    fill_panels(held, panels)
    for pair in range(spec_ref.shape[0]):
        table = pair_table(pair, place_ref, forward_ref)
        for turn, part in enumerate(table):
            table_ref[turn, pair] = part
        spec = spectrum_of(turned_patches(pair, place_ref, panels), table, stacked)
        spec_ref[pair] = spec
        wide_ref[pair] = spec.astype(jnp.float32)


def estimate(
    tile_refs, table_ref, corners_ref, spec_ref, usage_ref, forward_ref, rows0_ref, rows1_ref, rows2_ref, cols_ref,
     moments_ref, slopes_ref, panels, cross0, cross1, cross2, half0, half1, half2, plain,
    nested,
):
    def fill():
        if len(tile_refs) == 1:
            fill_panels(tile_refs[0], panels)
        else:
            odd = lax.axis_index("sec") & 1
            for parity, tile_ref in enumerate(tile_refs):
                pl.when(odd == parity)(functools.partial(fill_panels, tile_ref, panels))

    fill()
    groups = corners_ref.shape[1] // GROUP
    place_ref = Direct(corners_ref)
    quarter, eighth = PATCH // 4, PATCH // 8

    def packed(even, odd, width):
        lane = lax.broadcasted_iota(jnp.int32, even.shape, 1)
        return jnp.where((lane & (2 * width - 1)) < width, even, pltpu.roll(odd, width, 1))

    def cross_stage(group, slot):
        stacked = stacked_of(forward_ref)
        inner = []
        for pair in range(PAIRS):
            place = group * PAIRS + pair
            if table_ref is None:
                table = pair_table(place, place_ref, forward_ref)
            else:
                table = table_ref[0, place], table_ref[1, place]
            other = spectrum_of(turned_patches(place, place_ref, panels), table, stacked).astype(jnp.float32)
            own = spec_ref[place].astype(jnp.float32)
            own_real, own_imag = own[:, :PATCH], own[:, PATCH:]
            other_real, other_imag = other[:, :PATCH], other[:, PATCH:]
            real = own_real * other_real + own_imag * other_imag
            imag = own_imag * other_real - own_real * other_imag
            lanes = slice(pair % 2 * PATCH, (pair % 2 + 1) * PATCH)
            cross0[slot, pair // 2, :PATCH, lanes] = real.astype(jnp.bfloat16)
            cross0[slot, pair // 2, PATCH:, lanes] = imag.astype(jnp.bfloat16)
            inner.append(
                jnp.concatenate([real[:quarter], real[-quarter:], imag[:quarter], imag[-quarter:]], axis=0)
            )
        middle = [packed(inner[2 * turn], inner[2 * turn + 1], quarter) for turn in range(PAIRS // 2)]
        for turn in range(PAIRS // 2):
            cross1[slot, :, turn * PATCH : (turn + 1) * PATCH] = middle[turn].astype(jnp.bfloat16)
        inner = [
            jnp.concatenate(
                [part[:eighth], part[HALF - eighth : HALF], part[HALF : HALF + eighth], part[-eighth:]], axis=0
            )
            for part in middle
        ]
        cross2[slot] = packed(inner[0], inner[1], eighth).astype(jnp.bfloat16)

    def half_stage(source, slot):
        for turn in range(PAIRS // 2):
            half0[slot, turn] = product(rows0_ref[...], cross0[source, turn]).astype(jnp.bfloat16)
        half1[slot] = product(rows1_ref[...], cross1[source]).astype(jnp.bfloat16)
        half2[slot] = product(rows2_ref[...], cross2[source]).astype(jnp.bfloat16)

    def lines(half, tile):
        lanes = slice(tile * PATCH, (tile + 1) * PATCH)
        middle = half.shape[0] // 2
        return jnp.concatenate([half[:middle, lanes], half[middle:, lanes]], axis=1)

    def keep_ladder(level, group, members, correl):
        running, ladder = None, None
        for turn in range(PATCH // 8):
            row = (turn * 8 + HALF) % PATCH
            block = correl[row : row + 8]
            weight = block * block
            running = weight if running is None else running + weight
            ladder = running if ladder is None else ladder + running
        sublane = lax.broadcasted_iota(jnp.int32, running.shape, 0).astype(jnp.float32)
        by_col = jnp.sum(running, axis=0, keepdims=True)
        by_row = jnp.sum((HALF + sublane) * running - 8.0 * ladder, axis=0, keepdims=True)
        for turn, member in enumerate(members):
            lanes = slice(turn * PATCH, (turn + 1) * PATCH)
            place = group * GROUP + member
            plain[level, place : place + 1] = by_col[:, lanes]
            nested[level, place : place + 1] = by_row[:, lanes]

    def sums_stage(group, slot):
        correl = product(
            jnp.concatenate([lines(half0.at[slot, pair // 2], pair % 2) for pair in range(PAIRS)], axis=0), cols_ref[0]
        )
        for pair in range(PAIRS):
            keep_ladder(0, group, (2 * pair, 2 * pair + 1), correl[pair * PATCH : (pair + 1) * PATCH])
        line = jnp.concatenate([lines(half1.at[slot], turn) for turn in range(PAIRS // 2)], axis=0)
        for part in range(2):
            correl = product(line, cols_ref[1 + part])
            for turn in range(PAIRS // 2):
                pair = 2 * turn + part
                keep_ladder(1, group, (2 * pair, 2 * pair + 1), correl[turn * PATCH : (turn + 1) * PATCH])
        line = lines(half2.at[slot], 0)
        for part in range(2):
            correl = product(line, cols_ref[3 + part])
            for turn in range(2):
                total, slope = None, None
                for row in range(0, HALF, 8):
                    block = correl[row : row + 8, turn * PATCH : (turn + 1) * PATCH]
                    weight = block * block
                    sloped = weight * slopes_ref[row : row + 8]
                    total = weight if total is None else total + weight
                    slope = sloped if slope is None else slope + sloped
                total = jnp.sum(total, axis=0, keepdims=True)
                slope = jnp.sum(slope, axis=0, keepdims=True)
                for member in range(2):
                    place = group * GROUP + 4 * part + 2 * turn + member
                    plain[2, place : place + 1] = total
                    nested[2, place : place + 1] = slope

    for turn in range(groups + 4):
        if turn < groups:
            cross_stage(turn, turn % 4)
        if 3 <= turn <= groups + 2:
            half_stage((turn - 3) % 4, (turn - 1) % 2)
        if turn >= 4:
            sums_stage(turn - 4, turn % 2)

    usage = usage_ref[...].astype(jnp.float32)
    across = (((1,), (1,)), ((), ()))
    shape = plain.shape[1], PATCH
    own_lanes = (lax.broadcasted_iota(jnp.int32, shape, 1) >= HALF) == (
        (lax.broadcasted_iota(jnp.int32, shape, 0) & 1) == 1
    )
    along_rows, along_cols = 0.0, 0.0
    for level in range(LEVELS):
        by_col, by_row = plain[level], nested[level]
        if level == 2:
            by_col = jnp.where(own_lanes, by_col, 0.0)
            by_row = jnp.where(own_lanes, by_row, 0.0)
        col_part, row_part = (
            lax.dot_general(
                moments_ref[level // 2], part, across, precision=lax.Precision.HIGHEST,
                preferred_element_type=jnp.float32,
            )
            for part in (by_col, by_row)
        )
        scale = usage[level : level + 1] / (col_part[0:1] + 1e-6)
        along_rows = along_rows + row_part[2:3] * scale
        along_cols = along_cols + col_part[1:2] * scale
    count = jnp.maximum(jnp.sum(usage, axis=0, keepdims=True), 1.0)
    return jnp.concatenate([along_rows, along_cols], axis=0) / count


INS = 10


def next_kernel(*refs):
    ins, (tile_ref, table_ref, mask_ref, out_ref), scratch = refs[:INS], refs[INS : INS + 4], refs[INS + 4 :]
    message = jnp.concatenate([estimate([tile_ref], table_ref, *ins, *scratch), mask_ref[...].astype(jnp.float32)], axis=0)
    for section in range(out_ref.shape[0]):
        out_ref[section] = message


def skip_kernel(*refs):
    ins, tile_refs, out_ref, scratch = refs[:INS], refs[INS : INS + 2], refs[INS + 2], refs[INS + 3 :]
    out_ref[...] = estimate(tile_refs, None, *ins, *scratch)


def combine_kernel(shared_ref, skip_ref, *outs):
    me = lax.axis_index("sec")
    sections = shared_ref.shape[0]

    def mask_of(section):
        held = shared_ref[jnp.minimum(section, sections - 1), 2:3, :]
        return jnp.where(section < sections, held, jnp.zeros_like(held))

    def flow_of(section):
        return shared_ref[section, 0:2, :] * (mask_of(section) * mask_of(section + 1))

    flow_next = flow_of(me)
    outs[0][0] = flow_next
    outs[1][0] = skip_ref[...] * (mask_of(me) * mask_of(me + 2))
    outs[2][0] = lax.fori_loop(
        0, me, lambda section, held: held + flow_of(section), jnp.zeros_like(flow_next)
    ) + flow_next


def moved(block, axis, distance, receivers=(0, 1)):
    devices = range(lax.axis_size(axis))
    route = [(i + distance, i) for i in devices if i + distance in devices and i % 2 in receivers]
    return lax.ppermute(block, axis, route)


def on_device(section_tile, placement, tissue_mask, level_use):
    forward, *rest = tables()
    patches = placement.shape[0]
    side = section_tile.shape[1]
    tile = section_tile[0]
    sections = lax.axis_size("sec")
    vmem = pl.BlockSpec(memory_space=pltpu.VMEM)
    panels = (side // PATCH, side, PATCH)
    corners = placement.T
    spec = jax.ShapeDtypeStruct((patches // 2, PATCH, 2 * PATCH), jnp.bfloat16)
    sums = pltpu.VMEM((LEVELS, patches, PATCH), jnp.float32)

    def limit(mebibytes):
        return pltpu.CompilerParams(vmem_limit_bytes=mebibytes * 2**20)

    next_tile = moved(tile, "sec", 1)
    even_tile = moved(tile, "sec", 2, (0,))
    own_spec, wide_spec, col_tables = pl.pallas_call(
        own_kernel,
        out_shape=(
            spec,
            jax.ShapeDtypeStruct(spec.shape, jnp.float32),
            jax.ShapeDtypeStruct((2, patches // 2, 2 * PATCH, 2 * PATCH), jnp.bfloat16),
        ),
        in_specs=[pl.BlockSpec(memory_space=pltpu.HBM)] * 3,
        out_specs=(vmem, vmem, vmem),
        scratch_shapes=[
            pltpu.VMEM(tile.shape, tile.dtype),
            pltpu.VMEM(panels, jnp.float32),
            pltpu.VMEM(forward.shape, forward.dtype),
            pltpu.VMEM(corners.shape, corners.dtype),
            pltpu.SemaphoreType.DMA((3,)),
        ],
        compiler_params=limit(8),
        cost_estimate=pl.CostEstimate(flops=4 * 10**9, bytes_accessed=3 * 2**20, transcendentals=0),
        name="own_spectrum",
    )(*(pltpu.with_memory_space_constraint(array, pltpu.HBM) for array in (corners, tile, forward)))
    later_tile, own_spec = lax.optimization_barrier((tile, own_spec))
    odd_tile = moved(later_tile, "sec", 2, (1,))

    def flow(kernel, out_shape, own, *more):
        return pl.pallas_call(
            kernel,
            out_shape=jax.ShapeDtypeStruct(out_shape, jnp.float32),
            in_specs=[vmem] * (INS + len(more)),
            out_specs=vmem,
            scratch_shapes=[
                pltpu.VMEM(panels, jnp.float32),
                pltpu.VMEM((4, PAIRS // 2, 2 * PATCH, 2 * PATCH), jnp.bfloat16),
                pltpu.VMEM((4, PATCH, 2 * PATCH), jnp.bfloat16),
                pltpu.VMEM((4, HALF, PATCH), jnp.bfloat16),
                pltpu.VMEM((2, PAIRS // 2, 2 * PATCH, 2 * PATCH), jnp.bfloat16),
                pltpu.VMEM((2, 2 * PATCH, 2 * PATCH), jnp.bfloat16),
                pltpu.VMEM((2, PATCH, PATCH), jnp.bfloat16),
                sums,
                sums,
            ],
            compiler_params=limit(12),
            cost_estimate=pl.CostEstimate(flops=8 * 10**9, bytes_accessed=4 * 2**20, transcendentals=0),
        )(corners, own, level_use, forward, *rest, *more)

    message = flow(next_kernel, (sections, 3, patches), wide_spec, next_tile, col_tables, tissue_mask)
    shared = lax.all_to_all(message, "sec", 0, 0)
    flow_skip = flow(skip_kernel, (2, patches), own_spec, even_tile, odd_tile)
    out = jax.ShapeDtypeStruct((1, 2, patches), jnp.float32)
    return pl.pallas_call(
        combine_kernel,
        out_shape=(out, out, out),
        in_specs=[vmem, vmem],
        out_specs=(vmem, vmem, vmem),
        compiler_params=limit(2),
        name="combine",
    )(shared, flow_skip)


def solution(mesh):
    in_specs = (
        P(("grp", "sec"), None, None),
        P("grp", None),
        P(("grp", "sec"), None),
        P(None, "grp"),
    )
    out_specs = (
        P(("grp", "sec"), None, None),
        P(("grp", "sec"), None, None),
        P(("grp", "sec"), None, None),
    )

    return jax.shard_map(on_device, mesh=mesh, in_specs=in_specs, out_specs=out_specs, check_vma=False)
```

```python
import functools

import jax
import jax.numpy as jnp
import numpy as np
from jax import lax
from jax.experimental import pallas as pl
from jax.experimental.pallas import tpu as pltpu
from jax.sharding import PartitionSpec as P


PATCH = 128
LEVELS = 3
HALF = PATCH // 2
PAIRS = 4
GROUP = 2 * PAIRS


def tables():
    index = np.arange(PATCH)
    angles = ((index[:, None] * index[None, :]) % PATCH).astype(np.float32) * np.float32(2.0 * np.pi / PATCH)
    cosine = np.cos(angles).astype(jnp.bfloat16).astype(np.float32)
    sine = (-np.sin(angles)).astype(jnp.bfloat16).astype(np.float32)
    signed = np.minimum(index, PATCH - index)
    bands = [(signed < PATCH // 2 ** (level + 1)).astype(np.float32) for level in range(LEVELS)]
    offset = np.where(index < HALF, index, index - PATCH).astype(np.float64)

    cos_half, sin_half = cosine[:, :HALF], sine[:, :HALF]
    forward = np.concatenate(
        [
            np.tile(np.concatenate(part, axis=1), (2, 1))
            for part in ([cos_half, sin_half], [sin_half, cos_half])
        ]
        + [cosine / PATCH, sine / PATCH]
    )

    def inverse_rows(level, kept, points):
        left = (cosine * bands[level])[points][:, kept], (sine * bands[level])[points][:, kept]
        return np.block([[left[0], left[1]], [-left[1], left[0]]])

    def inverse_cols(level, width, lanes, members, points):
        twice = np.where(np.arange(width) == 0, 1.0, 2.0)[:, None] * bands[level][:width, None] / PATCH
        table = np.zeros((2 * PATCH, 2 * PATCH), np.float32)
        for turn, patch in enumerate(members):
            group = lanes.index(patch) * width
            cols = slice(turn * len(points), (turn + 1) * len(points))
            table[group : group + width, cols] = cosine[:width][:, points] * twice
            table[PATCH + group : PATCH + group + width, cols] = sine[:width][:, points] * twice
        return table

    quarter, eighth = PATCH // 4, PATCH // 8
    kept = [index, np.r_[:quarter, PATCH - quarter : PATCH], np.r_[:eighth, PATCH - eighth : PATCH]]
    coarse = index[::2]
    rows = [
        inverse_rows(0, kept[0], index),
        inverse_rows(1, kept[1], index),
        inverse_rows(2, kept[2], coarse),
    ]
    by_eighth = [0, 4, 2, 6, 1, 5, 3, 7]
    cols = np.stack(
        [
            inverse_cols(0, HALF, [0, 1], [0, 1], index),
            inverse_cols(1, quarter, [0, 2, 1, 3], [0, 1], index),
            inverse_cols(1, quarter, [0, 2, 1, 3], [2, 3], index),
            inverse_cols(2, eighth, by_eighth, [0, 1, 2, 3], coarse),
            inverse_cols(2, eighth, by_eighth, [4, 5, 6, 7], coarse),
        ]
    )

    spectrum = np.fft.fft(offset)
    spectrum[np.minimum(index, PATCH - index) >= quarter] = 0.0
    smooth = 2.0 * np.real(np.fft.ifft(spectrum))[::2]
    moments = np.zeros((2, 8, PATCH), np.float32)
    moments[0, 0], moments[0, 1], moments[0, 2] = 1.0, offset, 1.0
    moments[1, 0], moments[1, 1], moments[1, 2] = 4.0, 2.0 * np.tile(smooth, 2), 2.0
    slopes = np.broadcast_to(smooth[:, None], (HALF, PATCH)).astype(np.float32)
    return (
        jnp.asarray(forward),
        *(jnp.asarray(table, jnp.bfloat16) for table in rows),
        jnp.asarray(cols, jnp.bfloat16),
        jnp.asarray(moments),
        jnp.asarray(slopes),
    )


def product(left, right):
    return jnp.dot(left, right, preferred_element_type=jnp.float32)


def fill_panels(tile_ref, panels):
    for panel in range(panels.shape[0]):
        panels[panel] = tile_ref[:, panel * PATCH : (panel + 1) * PATCH].astype(jnp.float32)


def stacked_of(forward_ref):
    return forward_ref[forward_ref.shape[0] - 2 * PATCH :].astype(jnp.bfloat16)


class Direct:
    def __init__(self, corners_ref):
        self.values = corners_ref[...]

    def __getitem__(self, at):
        return self.values[at[0], at[1]]


def pair_table(pair, place_ref, forward_ref):
    lane = lax.broadcasted_iota(jnp.int32, (PATCH, PATCH), 1)
    table = []
    for member in range(2):
        shift = place_ref[1, 2 * pair + member] & (PATCH - 1)
        mine = (lane >= HALF) == (member == 1)
        parts = [
            jnp.where(mine, forward_ref[pl.ds((2 * order + 1) * PATCH - shift, PATCH), :], 0.0)
            for order in (member, 1 - member)
        ]
        table.append(jnp.concatenate(parts, axis=1).astype(jnp.bfloat16))
    table = jnp.concatenate(table, axis=0)
    return table, crossed(table)


def turned_patches(pair, place_ref, panels):
    last = panels.shape[0] - 1
    lane = lax.broadcasted_iota(jnp.int32, (PATCH, PATCH), 1)
    turned = []
    for member in range(2):
        row = place_ref[0, 2 * pair + member]
        col = place_ref[1, 2 * pair + member]
        panel = lax.shift_right_logical(col, PATCH.bit_length() - 1)
        here = panels[panel, pl.ds(row, PATCH), :]
        beside = panels[jnp.minimum(panel + 1, last), pl.ds(row, PATCH), :]
        turned.append(jnp.where(lane >= (col & (PATCH - 1)), here, beside).astype(jnp.bfloat16))
    return jnp.concatenate(turned, axis=1)


def crossed(parts):
    return jnp.concatenate([-parts[:, PATCH:], parts[:, :PATCH]], axis=1)


def spectrum_of(patches, table, stacked):
    rows = product(stacked, patches).astype(jnp.bfloat16)
    return (product(rows[:PATCH], table[0]) + product(rows[PATCH:], table[1]))


def own_kernel(corners_ref, tile_ref, tables_ref, spec_ref, wide_ref, table_ref, held, panels, forward_ref, corners, sems):
    copies = [
        pltpu.make_async_copy(source, target, sems.at[turn])
        for turn, (source, target) in enumerate(((tile_ref, held), (tables_ref, forward_ref), (corners_ref, corners)))
    ]
    for copy in copies:
        copy.start()
    for copy in copies:
        copy.wait()
    place_ref = Direct(corners)
    stacked = stacked_of(forward_ref)
    fill_panels(held, panels)
    for pair in range(spec_ref.shape[0]):
        table = pair_table(pair, place_ref, forward_ref)
        for turn, part in enumerate(table):
            table_ref[turn, pair] = part
        spec = spectrum_of(turned_patches(pair, place_ref, panels), table, stacked).astype(jnp.bfloat16)
        spec_ref[pair] = spec
        wide_ref[pair] = spec.astype(jnp.float32)


def estimate(
    tile_refs, table_ref, corners_ref, spec_ref, usage_ref, forward_ref, rows0_ref, rows1_ref, rows2_ref, cols_ref,
     moments_ref, slopes_ref, panels, cross0, cross1, cross2, half0, half1, half2, plain,
    nested,
):
    def fill():
        if len(tile_refs) == 1:
            fill_panels(tile_refs[0], panels)
        else:
            odd = lax.axis_index("sec") & 1
            for parity, tile_ref in enumerate(tile_refs):
                pl.when(odd == parity)(functools.partial(fill_panels, tile_ref, panels))

    fill()
    groups = corners_ref.shape[1] // GROUP
    place_ref = Direct(corners_ref)
    quarter, eighth = PATCH // 4, PATCH // 8

    def packed(even, odd, width):
        lane = lax.broadcasted_iota(jnp.int32, even.shape, 1)
        return jnp.where((lane & (2 * width - 1)) < width, even, pltpu.roll(odd, width, 1))

    def cross_stage(group, slot):
        stacked = stacked_of(forward_ref)
        inner = []
        for pair in range(PAIRS):
            place = group * PAIRS + pair
            if table_ref is None:
                table = pair_table(place, place_ref, forward_ref)
            else:
                table = table_ref[0, place], table_ref[1, place]
            other = spectrum_of(turned_patches(place, place_ref, panels), table, stacked)
            own = spec_ref[place].astype(jnp.float32)
            own_real, own_imag = own[:, :PATCH], own[:, PATCH:]
            other_real, other_imag = other[:, :PATCH], other[:, PATCH:]
            real = own_real * other_real + own_imag * other_imag
            imag = own_imag * other_real - own_real * other_imag
            lanes = slice(pair % 2 * PATCH, (pair % 2 + 1) * PATCH)
            cross0[slot, pair // 2, :PATCH, lanes] = real.astype(jnp.bfloat16)
            cross0[slot, pair // 2, PATCH:, lanes] = imag.astype(jnp.bfloat16)
            inner.append(
                jnp.concatenate([real[:quarter], real[-quarter:], imag[:quarter], imag[-quarter:]], axis=0)
            )
        middle = [packed(inner[2 * turn], inner[2 * turn + 1], quarter) for turn in range(PAIRS // 2)]
        for turn in range(PAIRS // 2):
            cross1[slot, :, turn * PATCH : (turn + 1) * PATCH] = middle[turn].astype(jnp.bfloat16)
        inner = [
            jnp.concatenate(
                [part[:eighth], part[HALF - eighth : HALF], part[HALF : HALF + eighth], part[-eighth:]], axis=0
            )
            for part in middle
        ]
        cross2[slot] = packed(inner[0], inner[1], eighth).astype(jnp.bfloat16)

    def half_stage(source, slot):
        for turn in range(PAIRS // 2):
            half0[slot, turn] = product(rows0_ref[...], cross0[source, turn]).astype(jnp.bfloat16)
        half1[slot] = product(rows1_ref[...], cross1[source]).astype(jnp.bfloat16)
        half2[slot] = product(rows2_ref[...], cross2[source]).astype(jnp.bfloat16)

    def lines(half, tile):
        lanes = slice(tile * PATCH, (tile + 1) * PATCH)
        middle = half.shape[0] // 2
        return jnp.concatenate([half[:middle, lanes], half[middle:, lanes]], axis=1)

    def keep_ladder(level, group, members, correl):
        running, ladder = None, None
        for turn in range(PATCH // 8):
            row = (turn * 8 + HALF) % PATCH
            block = correl[row : row + 8]
            weight = block * block
            running = weight if running is None else running + weight
            ladder = running if ladder is None else ladder + running
        sublane = lax.broadcasted_iota(jnp.int32, running.shape, 0).astype(jnp.float32)
        by_col = jnp.sum(running, axis=0, keepdims=True)
        by_row = jnp.sum((HALF + sublane) * running - 8.0 * ladder, axis=0, keepdims=True)
        for turn, member in enumerate(members):
            lanes = slice(turn * PATCH, (turn + 1) * PATCH)
            place = group * GROUP + member
            plain[level, place : place + 1] = by_col[:, lanes]
            nested[level, place : place + 1] = by_row[:, lanes]

    def sums_stage(group, slot):
        correl = product(
            jnp.concatenate([lines(half0.at[slot, pair // 2], pair % 2) for pair in range(PAIRS)], axis=0), cols_ref[0]
        )
        for pair in range(PAIRS):
            keep_ladder(0, group, (2 * pair, 2 * pair + 1), correl[pair * PATCH : (pair + 1) * PATCH])
        line = jnp.concatenate([lines(half1.at[slot], turn) for turn in range(PAIRS // 2)], axis=0)
        for part in range(2):
            correl = product(line, cols_ref[1 + part])
            for turn in range(PAIRS // 2):
                pair = 2 * turn + part
                keep_ladder(1, group, (2 * pair, 2 * pair + 1), correl[turn * PATCH : (turn + 1) * PATCH])
        line = lines(half2.at[slot], 0)
        for part in range(2):
            correl = product(line, cols_ref[3 + part])
            for turn in range(2):
                total, slope = None, None
                for row in range(0, HALF, 8):
                    block = correl[row : row + 8, turn * PATCH : (turn + 1) * PATCH]
                    weight = block * block
                    sloped = weight * slopes_ref[row : row + 8]
                    total = weight if total is None else total + weight
                    slope = sloped if slope is None else slope + sloped
                total = jnp.sum(total, axis=0, keepdims=True)
                slope = jnp.sum(slope, axis=0, keepdims=True)
                for member in range(2):
                    place = group * GROUP + 4 * part + 2 * turn + member
                    plain[2, place : place + 1] = total
                    nested[2, place : place + 1] = slope

    for turn in range(groups + 4):
        if turn < groups:
            cross_stage(turn, turn % 4)
        if 3 <= turn <= groups + 2:
            half_stage((turn - 3) % 4, (turn - 1) % 2)
        if turn >= 4:
            sums_stage(turn - 4, turn % 2)

    usage = usage_ref[...].astype(jnp.float32)
    across = (((1,), (1,)), ((), ()))
    shape = plain.shape[1], PATCH
    own_lanes = (lax.broadcasted_iota(jnp.int32, shape, 1) >= HALF) == (
        (lax.broadcasted_iota(jnp.int32, shape, 0) & 1) == 1
    )
    along_rows, along_cols = 0.0, 0.0
    for level in range(LEVELS):
        by_col, by_row = plain[level], nested[level]
        if level == 2:
            by_col = jnp.where(own_lanes, by_col, 0.0)
            by_row = jnp.where(own_lanes, by_row, 0.0)
        col_part, row_part = (
            lax.dot_general(
                moments_ref[level // 2], part, across, precision=lax.Precision.HIGHEST,
                preferred_element_type=jnp.float32,
            )
            for part in (by_col, by_row)
        )
        scale = usage[level : level + 1] / (col_part[0:1] + 1e-6)
        along_rows = along_rows + row_part[2:3] * scale
        along_cols = along_cols + col_part[1:2] * scale
    count = jnp.maximum(jnp.sum(usage, axis=0, keepdims=True), 1.0)
    return jnp.concatenate([along_rows, along_cols], axis=0) / count


INS = 10


def next_kernel(*refs):
    ins, (tile_ref, table_ref, mask_ref, out_ref), scratch = refs[:INS], refs[INS : INS + 4], refs[INS + 4 :]
    message = jnp.concatenate([estimate([tile_ref], table_ref, *ins, *scratch), mask_ref[...].astype(jnp.float32)], axis=0)
    for section in range(out_ref.shape[0]):
        out_ref[section] = message


def skip_kernel(*refs):
    ins, tile_refs, out_ref, scratch = refs[:INS], refs[INS : INS + 2], refs[INS + 2], refs[INS + 3 :]
    out_ref[...] = estimate(tile_refs, None, *ins, *scratch)


def combine_kernel(shared_ref, skip_ref, *outs):
    me = lax.axis_index("sec")
    sections = shared_ref.shape[0]

    def mask_of(section):
        held = shared_ref[jnp.minimum(section, sections - 1), 2:3, :]
        return jnp.where(section < sections, held, jnp.zeros_like(held))

    def flow_of(section):
        return shared_ref[section, 0:2, :] * (mask_of(section) * mask_of(section + 1))

    flow_next = flow_of(me)
    outs[0][0] = flow_next
    outs[1][0] = skip_ref[...] * (mask_of(me) * mask_of(me + 2))
    outs[2][0] = lax.fori_loop(
        0, me, lambda section, held: held + flow_of(section), jnp.zeros_like(flow_next)
    ) + flow_next


def moved(block, axis, distance, receivers=(0, 1)):
    devices = range(lax.axis_size(axis))
    route = [(i + distance, i) for i in devices if i + distance in devices and i % 2 in receivers]
    return lax.ppermute(block, axis, route)


def on_device(section_tile, placement, tissue_mask, level_use):
    forward, *rest = tables()
    patches = placement.shape[0]
    side = section_tile.shape[1]
    tile = section_tile[0]
    sections = lax.axis_size("sec")
    vmem = pl.BlockSpec(memory_space=pltpu.VMEM)
    panels = (side // PATCH, side, PATCH)
    corners = placement.T
    spec = jax.ShapeDtypeStruct((patches // 2, PATCH, 2 * PATCH), jnp.bfloat16)
    sums = pltpu.VMEM((LEVELS, patches, PATCH), jnp.float32)

    def limit(mebibytes):
        return pltpu.CompilerParams(vmem_limit_bytes=mebibytes * 2**20)

    next_tile = moved(tile, "sec", 1)
    even_tile = moved(tile, "sec", 2, (0,))
    own_spec, wide_spec, col_tables = pl.pallas_call(
        own_kernel,
        out_shape=(
            spec,
            jax.ShapeDtypeStruct(spec.shape, jnp.float32),
            jax.ShapeDtypeStruct((2, patches // 2, 2 * PATCH, 2 * PATCH), jnp.bfloat16),
        ),
        in_specs=[pl.BlockSpec(memory_space=pltpu.HBM)] * 3,
        out_specs=(vmem, vmem, vmem),
        scratch_shapes=[
            pltpu.VMEM(tile.shape, tile.dtype),
            pltpu.VMEM(panels, jnp.float32),
            pltpu.VMEM(forward.shape, forward.dtype),
            pltpu.VMEM(corners.shape, corners.dtype),
            pltpu.SemaphoreType.DMA((3,)),
        ],
        compiler_params=limit(8),
        cost_estimate=pl.CostEstimate(flops=4 * 10**9, bytes_accessed=3 * 2**20, transcendentals=0),
        name="own_spectrum",
    )(*(pltpu.with_memory_space_constraint(array, pltpu.HBM) for array in (corners, tile, forward)))
    later_tile, own_spec = lax.optimization_barrier((tile, own_spec))
    odd_tile = moved(later_tile, "sec", 2, (1,))

    def flow(kernel, out_shape, own, *more):
        return pl.pallas_call(
            kernel,
            out_shape=jax.ShapeDtypeStruct(out_shape, jnp.float32),
            in_specs=[vmem] * (INS + len(more)),
            out_specs=vmem,
            scratch_shapes=[
                pltpu.VMEM(panels, jnp.float32),
                pltpu.VMEM((4, PAIRS // 2, 2 * PATCH, 2 * PATCH), jnp.bfloat16),
                pltpu.VMEM((4, PATCH, 2 * PATCH), jnp.bfloat16),
                pltpu.VMEM((4, HALF, PATCH), jnp.bfloat16),
                pltpu.VMEM((2, PAIRS // 2, 2 * PATCH, 2 * PATCH), jnp.bfloat16),
                pltpu.VMEM((2, 2 * PATCH, 2 * PATCH), jnp.bfloat16),
                pltpu.VMEM((2, PATCH, PATCH), jnp.bfloat16),
                sums,
                sums,
            ],
            compiler_params=limit(12),
            cost_estimate=pl.CostEstimate(flops=8 * 10**9, bytes_accessed=4 * 2**20, transcendentals=0),
        )(corners, own, level_use, forward, *rest, *more)

    message = flow(next_kernel, (sections, 3, patches), wide_spec, next_tile, col_tables, tissue_mask)
    shared = lax.all_to_all(message, "sec", 0, 0)
    flow_skip = flow(skip_kernel, (2, patches), own_spec, even_tile, odd_tile)
    out = jax.ShapeDtypeStruct((1, 2, patches), jnp.float32)
    return pl.pallas_call(
        combine_kernel,
        out_shape=(out, out, out),
        in_specs=[vmem, vmem],
        out_specs=(vmem, vmem, vmem),
        compiler_params=limit(2),
        name="combine",
    )(shared, flow_skip)


def solution(mesh):
    in_specs = (
        P(("grp", "sec"), None, None),
        P("grp", None),
        P(("grp", "sec"), None),
        P(None, "grp"),
    )
    out_specs = (
        P(("grp", "sec"), None, None),
        P(("grp", "sec"), None, None),
        P(("grp", "sec"), None, None),
    )

    return jax.shard_map(on_device, mesh=mesh, in_specs=in_specs, out_specs=out_specs, check_vma=False)
```

```python
import functools

import jax
import jax.numpy as jnp
import numpy as np
from jax import lax
from jax.experimental import pallas as pl
from jax.experimental.pallas import tpu as pltpu
from jax.sharding import PartitionSpec as P


PATCH = 128
LEVELS = 3
HALF = PATCH // 2
PAIRS = 4
GROUP = 2 * PAIRS


def tables():
    index = np.arange(PATCH)
    angles = ((index[:, None] * index[None, :]) % PATCH).astype(np.float32) * np.float32(2.0 * np.pi / PATCH)
    cosine = np.cos(angles).astype(jnp.bfloat16).astype(np.float32)
    sine = (-np.sin(angles)).astype(jnp.bfloat16).astype(np.float32)
    signed = np.minimum(index, PATCH - index)
    bands = [(signed < PATCH // 2 ** (level + 1)).astype(np.float32) for level in range(LEVELS)]
    offset = np.where(index < HALF, index, index - PATCH).astype(np.float64)

    cos_half, sin_half = cosine[:, :HALF], sine[:, :HALF]
    forward = np.concatenate(
        [
            np.tile(np.concatenate(part, axis=1), (2, 1))
            for part in ([cos_half, sin_half], [sin_half, cos_half])
        ]
        + [cosine / PATCH, sine / PATCH]
    )

    def inverse_rows(level, kept, points):
        left = (cosine * bands[level])[points][:, kept], (sine * bands[level])[points][:, kept]
        return np.block([[left[0], left[1]], [-left[1], left[0]]])

    def inverse_cols(level, width, lanes, members, points):
        twice = np.where(np.arange(width) == 0, 1.0, 2.0)[:, None] * bands[level][:width, None] / PATCH
        table = np.zeros((2 * PATCH, 2 * PATCH), np.float32)
        for turn, patch in enumerate(members):
            group = lanes.index(patch) * width
            cols = slice(turn * len(points), (turn + 1) * len(points))
            table[group : group + width, cols] = cosine[:width][:, points] * twice
            table[PATCH + group : PATCH + group + width, cols] = sine[:width][:, points] * twice
        return table

    quarter, eighth = PATCH // 4, PATCH // 8
    kept = [index, np.r_[:quarter, PATCH - quarter : PATCH], np.r_[:eighth, PATCH - eighth : PATCH]]
    coarse = index[::2]
    rows = [
        inverse_rows(0, kept[0], index),
        inverse_rows(1, kept[1], index),
        inverse_rows(2, kept[2], coarse),
    ]
    by_eighth = [0, 4, 2, 6, 1, 5, 3, 7]
    cols = np.stack(
        [
            inverse_cols(0, HALF, [0, 1], [0, 1], index),
            inverse_cols(1, quarter, [0, 2, 1, 3], [0, 1], index),
            inverse_cols(1, quarter, [0, 2, 1, 3], [2, 3], index),
            inverse_cols(2, eighth, by_eighth, [0, 1, 2, 3], coarse),
            inverse_cols(2, eighth, by_eighth, [4, 5, 6, 7], coarse),
        ]
    )

    spectrum = np.fft.fft(offset)
    spectrum[np.minimum(index, PATCH - index) >= quarter] = 0.0
    smooth = 2.0 * np.real(np.fft.ifft(spectrum))[::2]
    moments = np.zeros((2, 8, PATCH), np.float32)
    moments[0, 0], moments[0, 1], moments[0, 2] = 1.0, offset, 1.0
    moments[1, 0], moments[1, 1], moments[1, 2] = 4.0, 2.0 * np.tile(smooth, 2), 2.0
    slopes = np.broadcast_to(smooth[:, None], (HALF, PATCH)).astype(np.float32)
    return (
        jnp.asarray(forward),
        *(jnp.asarray(table, jnp.bfloat16) for table in rows),
        jnp.asarray(cols, jnp.bfloat16),
        jnp.asarray(moments),
        jnp.asarray(slopes),
    )


def product(left, right):
    return jnp.dot(left, right, preferred_element_type=jnp.float32)


def fill_panels(tile_ref, panels):
    for panel in range(panels.shape[0]):
        panels[panel] = tile_ref[:, panel * PATCH : (panel + 1) * PATCH].astype(jnp.float32)


def transform_of(forward_ref):
    first = forward_ref.shape[0] - 2 * PATCH
    parts = [forward_ref[first + turn * PATCH : first + (turn + 1) * PATCH] for turn in range(2)]
    return jnp.concatenate(parts, axis=1).astype(jnp.bfloat16)


class Direct:
    def __init__(self, corners_ref):
        self.values = corners_ref[...]

    def __getitem__(self, at):
        return self.values[at[0], at[1]]


def pair_table(pair, place_ref, forward_ref):
    lane = lax.broadcasted_iota(jnp.int32, (PATCH, PATCH), 1)
    table = []
    for member in range(2):
        shift = place_ref[1, 2 * pair + member] & (PATCH - 1)
        mine = (lane >= HALF) == (member == 1)
        parts = [
            jnp.where(mine, forward_ref[pl.ds((2 * order + 1) * PATCH - shift, PATCH), :], 0.0)
            for order in (member, 1 - member)
        ]
        table.append(jnp.concatenate(parts, axis=1).astype(jnp.bfloat16))
    return jnp.concatenate(table, axis=0)


def turned_patches(pair, place_ref, panels):
    last = panels.shape[0] - 1
    lane = lax.broadcasted_iota(jnp.int32, (PATCH, PATCH), 1)
    turned = []
    for member in range(2):
        row = place_ref[0, 2 * pair + member]
        col = place_ref[1, 2 * pair + member]
        panel = lax.shift_right_logical(col, PATCH.bit_length() - 1)
        here = panels[panel, pl.ds(row, PATCH), :]
        beside = panels[jnp.minimum(panel + 1, last), pl.ds(row, PATCH), :]
        turned.append(jnp.where(lane >= (col & (PATCH - 1)), here, beside).astype(jnp.bfloat16))
    return jnp.concatenate(turned, axis=1)


def crossed(parts):
    return jnp.concatenate([-parts[:, PATCH:], parts[:, :PATCH]], axis=1)


def spectrum_by_columns(patches, table, forward):
    cols = product(patches, table).astype(jnp.bfloat16)
    return product(forward, jnp.concatenate([cols, crossed(cols)], axis=0)).astype(jnp.bfloat16)


def spectrum_by_rows(patches, table, stacked):
    rows = product(stacked, patches).astype(jnp.bfloat16)
    return (product(rows[:PATCH], table) + product(rows[PATCH:], crossed(table))).astype(jnp.bfloat16)


def own_kernel(corners_ref, tile_ref, tables_ref, spec_ref, wide_ref, table_ref, held, panels, forward_ref, corners, sems):
    copies = [
        pltpu.make_async_copy(source, target, sems.at[turn])
        for turn, (source, target) in enumerate(((tile_ref, held), (tables_ref, forward_ref), (corners_ref, corners)))
    ]
    for copy in copies:
        copy.start()
    for copy in copies:
        copy.wait()
    place_ref = Direct(corners)
    stacked = forward_ref[forward_ref.shape[0] - 2 * PATCH :].astype(jnp.bfloat16)
    fill_panels(held, panels)
    for pair in range(spec_ref.shape[0]):
        table = pair_table(pair, place_ref, forward_ref)
        table_ref[pair] = table
        spec = spectrum_by_rows(turned_patches(pair, place_ref, panels), table, stacked)
        spec_ref[pair] = spec
        wide_ref[pair] = spec.astype(jnp.float32)


def estimate(
    tile_refs, table_ref, corners_ref, spec_ref, usage_ref, forward_ref, rows0_ref, rows1_ref, rows2_ref, cols_ref,
     moments_ref, slopes_ref, panels, cross0, cross1, cross2, half0, half1, half2, plain,
    nested,
):
    def fill():
        if len(tile_refs) == 1:
            fill_panels(tile_refs[0], panels)
        else:
            odd = lax.axis_index("sec") & 1
            for parity, tile_ref in enumerate(tile_refs):
                pl.when(odd == parity)(functools.partial(fill_panels, tile_ref, panels))

    fill()
    groups = corners_ref.shape[1] // GROUP
    place_ref = Direct(corners_ref)
    quarter, eighth = PATCH // 4, PATCH // 8

    def packed(even, odd, width):
        lane = lax.broadcasted_iota(jnp.int32, even.shape, 1)
        return jnp.where((lane & (2 * width - 1)) < width, even, pltpu.roll(odd, width, 1))

    def cross_stage(group, slot):
        forward = transform_of(forward_ref)
        inner = []
        for pair in range(PAIRS):
            place = group * PAIRS + pair
            table = pair_table(place, place_ref, forward_ref) if table_ref is None else table_ref[place]
            other = spectrum_by_columns(turned_patches(place, place_ref, panels), table, forward).astype(jnp.float32)
            own = spec_ref[place].astype(jnp.float32)
            own_real, own_imag = own[:, :PATCH], own[:, PATCH:]
            other_real, other_imag = other[:, :PATCH], other[:, PATCH:]
            real = own_real * other_real + own_imag * other_imag
            imag = own_imag * other_real - own_real * other_imag
            lanes = slice(pair % 2 * PATCH, (pair % 2 + 1) * PATCH)
            cross0[slot, pair // 2, :PATCH, lanes] = real.astype(jnp.bfloat16)
            cross0[slot, pair // 2, PATCH:, lanes] = imag.astype(jnp.bfloat16)
            inner.append(
                jnp.concatenate([real[:quarter], real[-quarter:], imag[:quarter], imag[-quarter:]], axis=0)
            )
        middle = [packed(inner[2 * turn], inner[2 * turn + 1], quarter) for turn in range(PAIRS // 2)]
        for turn in range(PAIRS // 2):
            cross1[slot, :, turn * PATCH : (turn + 1) * PATCH] = middle[turn].astype(jnp.bfloat16)
        inner = [
            jnp.concatenate(
                [part[:eighth], part[HALF - eighth : HALF], part[HALF : HALF + eighth], part[-eighth:]], axis=0
            )
            for part in middle
        ]
        cross2[slot] = packed(inner[0], inner[1], eighth).astype(jnp.bfloat16)

    def half_stage(source, slot):
        for turn in range(PAIRS // 2):
            half0[slot, turn] = product(rows0_ref[...], cross0[source, turn]).astype(jnp.bfloat16)
        half1[slot] = product(rows1_ref[...], cross1[source]).astype(jnp.bfloat16)
        half2[slot] = product(rows2_ref[...], cross2[source]).astype(jnp.bfloat16)

    def lines(half, tile):
        lanes = slice(tile * PATCH, (tile + 1) * PATCH)
        middle = half.shape[0] // 2
        return jnp.concatenate([half[:middle, lanes], half[middle:, lanes]], axis=1)

    def keep_ladder(level, group, members, correl):
        running, ladder = None, None
        for turn in range(PATCH // 8):
            row = (turn * 8 + HALF) % PATCH
            block = correl[row : row + 8]
            weight = block * block
            running = weight if running is None else running + weight
            ladder = running if ladder is None else ladder + running
        sublane = lax.broadcasted_iota(jnp.int32, running.shape, 0).astype(jnp.float32)
        by_col = jnp.sum(running, axis=0, keepdims=True)
        by_row = jnp.sum((HALF + sublane) * running - 8.0 * ladder, axis=0, keepdims=True)
        for turn, member in enumerate(members):
            lanes = slice(turn * PATCH, (turn + 1) * PATCH)
            place = group * GROUP + member
            plain[level, place : place + 1] = by_col[:, lanes]
            nested[level, place : place + 1] = by_row[:, lanes]

    def sums_stage(group, slot):
        correl = product(
            jnp.concatenate([lines(half0.at[slot, pair // 2], pair % 2) for pair in range(PAIRS)], axis=0), cols_ref[0]
        )
        for pair in range(PAIRS):
            keep_ladder(0, group, (2 * pair, 2 * pair + 1), correl[pair * PATCH : (pair + 1) * PATCH])
        line = jnp.concatenate([lines(half1.at[slot], turn) for turn in range(PAIRS // 2)], axis=0)
        for part in range(2):
            correl = product(line, cols_ref[1 + part])
            for turn in range(PAIRS // 2):
                pair = 2 * turn + part
                keep_ladder(1, group, (2 * pair, 2 * pair + 1), correl[turn * PATCH : (turn + 1) * PATCH])
        line = lines(half2.at[slot], 0)
        for part in range(2):
            correl = product(line, cols_ref[3 + part])
            for turn in range(2):
                total, slope = None, None
                for row in range(0, HALF, 8):
                    block = correl[row : row + 8, turn * PATCH : (turn + 1) * PATCH]
                    weight = block * block
                    sloped = weight * slopes_ref[row : row + 8]
                    total = weight if total is None else total + weight
                    slope = sloped if slope is None else slope + sloped
                total = jnp.sum(total, axis=0, keepdims=True)
                slope = jnp.sum(slope, axis=0, keepdims=True)
                for member in range(2):
                    place = group * GROUP + 4 * part + 2 * turn + member
                    plain[2, place : place + 1] = total
                    nested[2, place : place + 1] = slope

    for turn in range(groups + 4):
        if turn < groups:
            cross_stage(turn, turn % 4)
        if 3 <= turn <= groups + 2:
            half_stage((turn - 3) % 4, (turn - 1) % 2)
        if turn >= 4:
            sums_stage(turn - 4, turn % 2)

    usage = usage_ref[...].astype(jnp.float32)
    across = (((1,), (1,)), ((), ()))
    shape = plain.shape[1], PATCH
    own_lanes = (lax.broadcasted_iota(jnp.int32, shape, 1) >= HALF) == (
        (lax.broadcasted_iota(jnp.int32, shape, 0) & 1) == 1
    )
    along_rows, along_cols = 0.0, 0.0
    for level in range(LEVELS):
        by_col, by_row = plain[level], nested[level]
        if level == 2:
            by_col = jnp.where(own_lanes, by_col, 0.0)
            by_row = jnp.where(own_lanes, by_row, 0.0)
        col_part, row_part = (
            lax.dot_general(
                moments_ref[level // 2], part, across, precision=lax.Precision.HIGHEST,
                preferred_element_type=jnp.float32,
            )
            for part in (by_col, by_row)
        )
        scale = usage[level : level + 1] / (col_part[0:1] + 1e-6)
        along_rows = along_rows + row_part[2:3] * scale
        along_cols = along_cols + col_part[1:2] * scale
    count = jnp.maximum(jnp.sum(usage, axis=0, keepdims=True), 1.0)
    return jnp.concatenate([along_rows, along_cols], axis=0) / count


INS = 10


def next_kernel(*refs):
    ins, (tile_ref, table_ref, mask_ref, out_ref), scratch = refs[:INS], refs[INS : INS + 4], refs[INS + 4 :]
    message = jnp.concatenate([estimate([tile_ref], table_ref, *ins, *scratch), mask_ref[...].astype(jnp.float32)], axis=0)
    for section in range(out_ref.shape[0]):
        out_ref[section] = message


def skip_kernel(*refs):
    ins, tile_refs, out_ref, scratch = refs[:INS], refs[INS : INS + 2], refs[INS + 2], refs[INS + 3 :]
    out_ref[...] = estimate(tile_refs, None, *ins, *scratch)


def combine_kernel(shared_ref, skip_ref, *outs):
    me = lax.axis_index("sec")
    sections = shared_ref.shape[0]

    def mask_of(section):
        held = shared_ref[jnp.minimum(section, sections - 1), 2:3, :]
        return jnp.where(section < sections, held, jnp.zeros_like(held))

    def flow_of(section):
        return shared_ref[section, 0:2, :] * (mask_of(section) * mask_of(section + 1))

    flow_next = flow_of(me)
    outs[0][0] = flow_next
    outs[1][0] = skip_ref[...] * (mask_of(me) * mask_of(me + 2))
    outs[2][0] = lax.fori_loop(
        0, me, lambda section, held: held + flow_of(section), jnp.zeros_like(flow_next)
    ) + flow_next


def moved(block, axis, distance, receivers=(0, 1)):
    devices = range(lax.axis_size(axis))
    route = [(i + distance, i) for i in devices if i + distance in devices and i % 2 in receivers]
    return lax.ppermute(block, axis, route)


def on_device(section_tile, placement, tissue_mask, level_use):
    forward, *rest = tables()
    patches = placement.shape[0]
    side = section_tile.shape[1]
    tile = section_tile[0]
    sections = lax.axis_size("sec")
    vmem = pl.BlockSpec(memory_space=pltpu.VMEM)
    panels = (side // PATCH, side, PATCH)
    corners = placement.T
    spec = jax.ShapeDtypeStruct((patches // 2, PATCH, 2 * PATCH), jnp.bfloat16)
    sums = pltpu.VMEM((LEVELS, patches, PATCH), jnp.float32)

    def limit(mebibytes):
        return pltpu.CompilerParams(vmem_limit_bytes=mebibytes * 2**20)

    next_tile = moved(tile, "sec", 1)
    even_tile = moved(tile, "sec", 2, (0,))
    own_spec, wide_spec, col_tables = pl.pallas_call(
        own_kernel,
        out_shape=(
            spec,
            jax.ShapeDtypeStruct(spec.shape, jnp.float32),
            jax.ShapeDtypeStruct((patches // 2, 2 * PATCH, 2 * PATCH), jnp.bfloat16),
        ),
        in_specs=[pl.BlockSpec(memory_space=pltpu.HBM)] * 3,
        out_specs=(vmem, vmem, vmem),
        scratch_shapes=[
            pltpu.VMEM(tile.shape, tile.dtype),
            pltpu.VMEM(panels, jnp.float32),
            pltpu.VMEM(forward.shape, forward.dtype),
            pltpu.VMEM(corners.shape, corners.dtype),
            pltpu.SemaphoreType.DMA((3,)),
        ],
        compiler_params=limit(8),
        cost_estimate=pl.CostEstimate(flops=4 * 10**9, bytes_accessed=3 * 2**20, transcendentals=0),
        name="own_spectrum",
    )(*(pltpu.with_memory_space_constraint(array, pltpu.HBM) for array in (corners, tile, forward)))
    later_tile, own_spec = lax.optimization_barrier((tile, own_spec))
    odd_tile = moved(later_tile, "sec", 2, (1,))

    def flow(kernel, out_shape, own, *more):
        return pl.pallas_call(
            kernel,
            out_shape=jax.ShapeDtypeStruct(out_shape, jnp.float32),
            in_specs=[vmem] * (INS + len(more)),
            out_specs=vmem,
            scratch_shapes=[
                pltpu.VMEM(panels, jnp.float32),
                pltpu.VMEM((4, PAIRS // 2, 2 * PATCH, 2 * PATCH), jnp.bfloat16),
                pltpu.VMEM((4, PATCH, 2 * PATCH), jnp.bfloat16),
                pltpu.VMEM((4, HALF, PATCH), jnp.bfloat16),
                pltpu.VMEM((2, PAIRS // 2, 2 * PATCH, 2 * PATCH), jnp.bfloat16),
                pltpu.VMEM((2, 2 * PATCH, 2 * PATCH), jnp.bfloat16),
                pltpu.VMEM((2, PATCH, PATCH), jnp.bfloat16),
                sums,
                sums,
            ],
            compiler_params=limit(12),
            cost_estimate=pl.CostEstimate(flops=8 * 10**9, bytes_accessed=4 * 2**20, transcendentals=0),
        )(corners, own, level_use, forward, *rest, *more)

    message = flow(next_kernel, (sections, 3, patches), wide_spec, next_tile, col_tables, tissue_mask)
    shared = lax.all_to_all(message, "sec", 0, 0)
    flow_skip = flow(skip_kernel, (2, patches), own_spec, even_tile, odd_tile)
    out = jax.ShapeDtypeStruct((1, 2, patches), jnp.float32)
    return pl.pallas_call(
        combine_kernel,
        out_shape=(out, out, out),
        in_specs=[vmem, vmem],
        out_specs=(vmem, vmem, vmem),
        compiler_params=limit(2),
        name="combine",
    )(shared, flow_skip)


def solution(mesh):
    in_specs = (
        P(("grp", "sec"), None, None),
        P("grp", None),
        P(("grp", "sec"), None),
        P(None, "grp"),
    )
    out_specs = (
        P(("grp", "sec"), None, None),
        P(("grp", "sec"), None, None),
        P(("grp", "sec"), None, None),
    )

    return jax.shard_map(on_device, mesh=mesh, in_specs=in_specs, out_specs=out_specs, check_vma=False)
```
